512 devices in a mesh: expert: 32 (over z, core), row: 16 (over y, x).
Axes of the slice: x: 4, y: 4, z: 16, core: 2. Of those that a mesh axis runs over, the one named last changes fastest.
Arguments:
- grads: bfloat16 [32, 7168, 2048], P('expert', 'row')
- basis: bfloat16 [32, 7168, 256], P('expert', 'row'), may hold values from -0.0625 to 0.0625
- loads: int32 [32], P('expert'), may hold values from 1 to 1, as said below
- flags: int32 [32], P('expert'), may hold values 0 or 1
Outputs:
- new_basis: float32 [32, 7168, 256], P('expert', 'row')
- rotated: float32 [32, 256, 2048], P('expert', None, 'row')
The draws below stay inside these ranges and needn't reach their ends.
Inputs may be any that keep to these rules, and one draw needn't show every extreme that they name: Slots 0 to loads[d] - 1 of expert-axis index d are live and hold experts; the others are empty. Some index has all 1 slots live.
All inputs are finite; a program needn't handle non-finite values. No bound on the sum of `flags` on one device may be relied on, other than what follows from the above.
Results may differ from the reference program's by a relative error of at most 0.006.
Values sent between devices are 32-bit elements; how exact they have to be, the bound alone decides.
No kernel may reach another device: no remote copies, remote signals or barrier semaphores. Data moves between devices by JAX's collectives and lax.ppermute only.
A program may use at most 64 MiB of HBM per device.

```python
import math
import jax
import jax.numpy as jnp
from jax import lax

D = 7168
S = 2048
K = 256
SLOTS = 1
EXPERTS = 32


def draw_grads(key, part):
    first_key, second_key = jax.random.split(jax.random.fold_in(key, 7))
    entries = jax.random.normal(first_key, (EXPERTS, D, S), jnp.float32)
    row_scale = jnp.exp(jax.random.uniform(second_key, (EXPERTS, D, 1), jnp.float32, math.log(0.5), math.log(5.0)))
    expert_ramp = 1.0 + 2.0 * jnp.arange(EXPERTS, dtype=jnp.float32) / max(EXPERTS - 1, 1)
    row_ramp = 1.0 + 2.0 * jnp.arange(D, dtype=jnp.float32) / (D - 1)
    factor = jnp.sqrt(expert_ramp)[:, None, None] * jnp.sqrt(row_ramp)[None, :, None]
    return (entries * row_scale * factor).astype(jnp.bfloat16)


def draw_loads(key, part):
    device_count = EXPERTS // SLOTS
    first_key, second_key = jax.random.split(jax.random.fold_in(key, 3))
    counts = jax.random.randint(first_key, (device_count,), 1, SLOTS + 1)
    chosen = jax.random.randint(second_key, (), 0, device_count)
    return jnp.where(jnp.arange(device_count) == chosen, SLOTS, counts).astype(jnp.int32)


def touch_ends(values, stream_key, smallest, high):
    extent = values.shape
    place = [jax.random.randint(jax.random.fold_in(stream_key, axis), (), 0, extent[axis]) for axis in range(len(extent))]
    values = values.at[tuple(place)].set(smallest)
    longest = extent.index(max(extent))
    place[longest] = (place[longest] + 1) % extent[longest]
    return values.at[tuple(place)].set(high)


def level_of(key, shape, cuts, smallest, top_value):
    factor_of, own = 1.0, jax.random.fold_in(key, 6)
    for axis_at, blocks in cuts:
        steps = jnp.exp(jax.random.uniform(jax.random.fold_in(own, axis_at), (blocks,), jnp.float32, smallest / len(cuts), top_value / len(cuts)))
        factor_of = factor_of * jnp.repeat(steps, shape[axis_at] // blocks).reshape([-1 if axis == axis_at else 1 for axis in range(len(shape))])
    return factor_of


def scatter_about(rng, shape, width, reach, cuts=(), kind=jnp.bfloat16):
    result = width * jax.random.normal(rng, shape, jnp.float32)
    if cuts:
        result = result * level_of(rng, shape, cuts, -0.22, 0.18)
    return jnp.clip(result, -reach, reach).astype(kind)


def setup_inputs(seed: int = 0) -> dict:
    streams_of = jax.random.split(jax.random.key(seed), 5)
    return {
        "grads": draw_grads(jax.random.fold_in(streams_of[4], 71), 0),
        "basis": scatter_about(streams_of[1], (EXPERTS, D, K), D ** -0.5, 0.0625, ((0, 32), (1, 16))),
        "loads": draw_loads(jax.random.fold_in(streams_of[4], 71), 0),
        "flags": touch_ends((jax.random.randint(streams_of[3], (EXPERTS,), 0, 2) < 1).astype(jnp.int32), jax.random.fold_in(streams_of[3], 1), 0, 1),
    }


def reference(grads, basis, loads, flags):
    expert_total = grads.shape[0]
    slot_count = expert_total // loads.shape[0]
    expert_ids = jnp.arange(expert_total, dtype=jnp.int32)
    live_mask = expert_ids % slot_count < loads[expert_ids // slot_count]
    refresh = jnp.logical_and(live_mask, flags == 1)

    def square_sum(expert):
        gradient = grads[expert].astype(jnp.float32)
        return jnp.sum(gradient * gradient)
    square_sums = lax.map(square_sum, expert_ids)
    total_sq = jnp.sum(jnp.where(live_mask, square_sums, 0.0))
    live_count = jnp.sum(live_mask.astype(jnp.float32))
    norm_scale = lax.rsqrt(total_sq / (live_count * D * S) + 1e-06)

    def refresh_one(expert):
        gradient = grads[expert]
        old_basis = basis[expert]
        inner_sum = jnp.dot(gradient.T.astype(jnp.float32), old_basis.astype(jnp.float32), preferred_element_type=jnp.float32).astype(jnp.bfloat16)
        power_rows = jnp.dot(gradient.astype(jnp.float32), inner_sum.astype(jnp.float32), preferred_element_type=jnp.float32).astype(jnp.bfloat16)
        ortho, upper = jnp.linalg.qr(power_rows.astype(jnp.float32))
        signs = jnp.where(jnp.diagonal(upper) < 0, -1.0, 1.0).astype(ortho.dtype)
        ortho = ortho * signs[None, :]
        fresh_rot = jnp.dot(ortho.T, gradient.astype(jnp.float32), precision=lax.Precision.HIGHEST)
        stale_rot = jnp.dot(old_basis.T.astype(jnp.float32), gradient.astype(jnp.float32), preferred_element_type=jnp.float32)
        basis_out = jnp.where(refresh[expert], ortho, jnp.where(live_mask[expert], old_basis.astype(jnp.float32), 0.0))
        rotated_out = jnp.where(refresh[expert], fresh_rot, jnp.where(live_mask[expert], stale_rot, 0.0)) * norm_scale
        return (basis_out, rotated_out)
    new_basis, rotated = lax.map(refresh_one, expert_ids)
    return (new_basis, rotated)
```

```python
import functools

import jax
import jax.numpy as jnp
from jax import lax
from jax.experimental import pallas as pl
from jax.experimental.pallas import tpu as pltpu
from jax.sharding import Mesh
from jax.sharding import PartitionSpec as P

ROW = ("row_0", "row_1")
EXPERT = ("expert_0", "expert_1")
F32 = jnp.float32
BF16 = jnp.bfloat16
HIGH = lax.Precision.HIGHEST
BLOCK = 32
NT = (((1,), (1,)), ((), ()))
TN = (((0,), (0,)), ((), ()))
VM = pl.BlockSpec(memory_space=pltpu.VMEM)
SM = pl.BlockSpec(memory_space=pltpu.SMEM)


def cost(flops, nbytes):
    return pl.CostEstimate(flops=int(flops), bytes_accessed=int(nbytes), transcendentals=0)


def product_kernel(extra, left_ref, g_ref, out_ref, lt_ref):
    @pl.when(pl.program_id(0) == 0)
    def _():
        lt_ref[...] = left_ref[...].astype(F32).T.astype(BF16)

    k = lt_ref.shape[0]
    both = jnp.dot(lt_ref[...], g_ref[...], preferred_element_type=F32)
    for h in range(2):
        out_ref[h, :k, :] = both[:, 128 * h : 128 * (h + 1)]
        if extra:
            part = g_ref[:, 128 * h : 128 * (h + 1)].astype(F32)
            out_ref[h, k:, :] = (part * part).reshape(-1, 8, 128).sum(axis=0)


def product(left, g, extra):
    d, k = left.shape
    s = g.shape[1]
    rows = k + extra
    return pl.pallas_call(
        functools.partial(product_kernel, extra),
        grid=(s // 256,),
        in_specs=[pl.BlockSpec((d, k), lambda i: (0, 0)), pl.BlockSpec((d, 256), lambda i: (0, i))],
        out_specs=pl.BlockSpec((2, rows, 128), lambda i: (i, 0, 0)),
        out_shape=jax.ShapeDtypeStruct((s // 128, rows, 128), F32),
        scratch_shapes=[pltpu.VMEM((k, d), BF16)],
        cost_estimate=cost(2 * d * k * s, 2 * d * (s + k) + 4 * rows * s),
        name="product",
    )(left, g)


def spread_kernel(in_ref, out_ref, own_ref):
    total = in_ref[...].sum(axis=0)
    own_ref[...] = total
    out_ref[...] = jnp.broadcast_to(total[None], out_ref.shape)


def spread(parts, steps):
    n, r, c = parts.shape
    b = r // steps
    return pl.pallas_call(
        spread_kernel,
        grid=(steps,),
        in_specs=[pl.BlockSpec((n, b, c), lambda i: (0, i, 0))],
        out_specs=[pl.BlockSpec((n, b, c), lambda i: (0, i, 0)), pl.BlockSpec((b, c), lambda i: (i, 0))],
        out_shape=[jax.ShapeDtypeStruct(parts.shape, F32), jax.ShapeDtypeStruct((r, c), F32)],
        cost_estimate=cost(n * r * c, 8 * n * r * c),
        name="spread",
    )(parts)


def power_of_two(m):
    s = jnp.ones_like(m)
    for e in (64, 32, 16, 8, 4, 2, 1):
        big = m >= 2.0**e
        s = jnp.where(big, s * 2.0**-e, s)
        m = jnp.where(big, m * 2.0**-e, m)
    for e in (64, 32, 16, 8, 4, 2, 1):
        small = m < 2.0 ** (1 - e)
        s = jnp.where(small, s * 2.0 ** (e - 1), s)
        m = jnp.where(small, m * 2.0 ** (e - 1), m)
    return s


def power_kernel(g_ref, w_ref, p_ref, gram_ref, sq_ref):
    n = w_ref.shape[0]
    k = p_ref.shape[1]
    m = jnp.abs(w_ref[0, :k, :])
    sq = w_ref[0, k:, :]
    for j in range(1, n):
        m = jnp.maximum(m, jnp.abs(w_ref[j, :k, :]))
        sq = sq + w_ref[j, k:, :]
    sq_ref[...] = sq
    scale = power_of_two(jnp.max(m, axis=1, keepdims=True))
    acc = jnp.zeros(p_ref.shape, F32)
    for j in range(0, n, 2):
        w = jnp.concatenate([w_ref[j, :k, :], w_ref[j + 1, :k, :]], axis=1)
        w = (w * scale).astype(BF16)
        acc = acc + lax.dot_general(g_ref[:, 128 * j : 128 * j + 256], w, NT, preferred_element_type=F32)
    p = acc.astype(BF16)
    p_ref[...] = p
    pt = p.astype(F32).T.astype(BF16)
    gram_ref[...] = jnp.dot(pt, p, preferred_element_type=F32)


def power(g, w, k):
    d, s = g.shape
    return pl.pallas_call(
        power_kernel,
        in_specs=[VM, VM],
        out_specs=[VM, VM, VM],
        out_shape=[
            jax.ShapeDtypeStruct((d, k), BF16),
            jax.ShapeDtypeStruct((k, k), F32),
            jax.ShapeDtypeStruct((w.shape[1] - k, 128), F32),
        ],
        cost_estimate=cost(2 * d * k * s, 2 * d * s + 4 * k * s),
        name="power",
    )(g, w)


def sub(v, r):
    return jnp.broadcast_to(v[r : r + 1, :], v.shape)


def small_inverse(d):
    groups = BLOCK // 8
    row = lax.broadcasted_iota(jnp.int32, (8, 128), 0)
    lane = lax.broadcasted_iota(jnp.int32, (8, 128), 1)
    x = [jnp.where(lane == row + 8 * g, 1.0, 0.0) for g in range(groups)]
    c = [
        {g: jnp.broadcast_to(d[8 * g : 8 * g + 8, k : k + 1], (8, 128)) for g in range(k // 8, groups)}
        for k in range(BLOCK)
    ]
    for j in range(BLOCK):
        gj, sj = j // 8, j % 8
        r = lax.rsqrt(sub(c[j][gj], sj))
        low = {g: c[j][g] * r for g in range(gj, groups)}
        for k in range(j + 1, BLOCK):
            at = sub(low[k // 8], k % 8)
            for g in range(k // 8, groups):
                c[k][g] = c[k][g] - low[g] * at
        xr = sub(x[gj], sj) * r
        below = jnp.where(row > sj, low[gj], 0.0)
        x[gj] = jnp.where(row == sj, xr, x[gj] - below * xr)
        for g in range(gj + 1, groups):
            x[g] = x[g] - low[g] * xr
    return jnp.concatenate(x, axis=0)


def factor_kernel(refresh_ref, a_ref, p_ref, basis_ref, inv_ref, new_ref, t_ref):
    k = inv_ref.shape[0]
    a = a_ref[...].reshape(k, k)
    lane = lax.broadcasted_iota(jnp.int32, (BLOCK, k), 1)
    row = lax.broadcasted_iota(jnp.int32, (BLOCK, k), 0)
    for b in range(k // BLOCK):
        lo = b * BLOCK
        hi = lo + BLOCK
        r = jnp.where(lane >= lo, a[lo:hi, :], 0.0)
        if b:
            t = t_ref[:lo, :]
            at_lane = lax.broadcasted_iota(jnp.int32, (lo, k), 1)
            at_row = lax.broadcasted_iota(jnp.int32, (lo, k), 0)
            tm = jnp.where(jnp.logical_and(at_lane < lo, at_row < at_lane), 0.0, t)
            r = r - lax.dot_general(t[:, lo:hi], tm, TN, precision=HIGH, preferred_element_type=F32)
        x = small_inverse(r[:, lo:hi])[:, :BLOCK]
        inside = jnp.logical_and(lane >= lo, lane < hi)
        r = jnp.where(inside, jnp.where(lane - lo == row, 1.0, 0.0), r)
        t_ref[lo:hi, :] = jnp.dot(x, r, precision=HIGH, preferred_element_type=F32)
    whole_lane = lax.broadcasted_iota(jnp.int32, (k, k), 1)
    whole_row = lax.broadcasted_iota(jnp.int32, (k, k), 0)
    inv = jnp.where(whole_lane <= whole_row, t_ref[...], 0.0)
    inv_ref[...] = inv
    fresh = lax.dot_general(p_ref[...].astype(F32), inv, NT, precision=HIGH, preferred_element_type=F32)
    old = jnp.where(refresh_ref[1] > 0, basis_ref[...].astype(F32), 0.0)
    new_ref[...] = jnp.where(refresh_ref[0] > 0, fresh, old)


def factor(state, gram, p, basis):
    d, k = p.shape
    return pl.pallas_call(
        factor_kernel,
        in_specs=[SM, VM, VM, VM],
        out_specs=[VM, VM],
        out_shape=[jax.ShapeDtypeStruct((k, k), F32), jax.ShapeDtypeStruct((d, k), F32)],
        scratch_shapes=[pltpu.VMEM((k, k), F32)],
        cost_estimate=cost(6e9, 4 * d * k),
        name="factor",
    )(state, gram, p, basis)


def rotate_kernel(state_ref, scale_ref, parts_ref, inv_ref, stale_ref, out_ref):
    cross = parts_ref[...].sum(axis=0)
    fresh = jnp.dot(inv_ref[...], cross, precision=HIGH, preferred_element_type=F32)
    k = out_ref.shape[0]
    old = jnp.where(state_ref[1] > 0, stale_ref[:k, :], 0.0)
    out_ref[...] = jnp.where(state_ref[0] > 0, fresh, old) * scale_ref[0]


def rotate(state, scale, parts, inv, stale):
    n, k, c = parts.shape
    return pl.pallas_call(
        rotate_kernel,
        in_specs=[SM, SM, VM, VM, VM],
        out_specs=VM,
        out_shape=jax.ShapeDtypeStruct((k, c), F32),
        cost_estimate=cost(2 * k * k * c, 4 * n * k * c),
        name="rotate",
    )(state, scale, parts, inv, stale)


def exchange(blocks, axes):
    return lax.all_to_all(blocks, axes, split_axis=0, concat_axis=0, tiled=True)


def on_device(d_whole, grads, basis, loads, flags):
    g, b = grads[0], basis[0]
    k = b.shape[1]
    s = g.shape[1]
    live = loads[0] >= 1
    refresh = jnp.logical_and(live, flags[0] == 1)
    state = jnp.stack([refresh, live]).astype(jnp.int32)

    parts = product(b, g, 8)
    copies, stale = spread(exchange(parts, ROW), 3)
    p, gram, squares = power(g, exchange(copies, ROW), k)

    n = parts.shape[0]
    gram_copies, _ = spread(exchange(gram.reshape(n, k // n, k), ROW), 1)
    cross = product(p, g, 0)
    whole_gram = exchange(gram_copies, ROW)

    own = jnp.stack([jnp.where(live, squares.sum(), 0.0), live.astype(F32)])
    experts = lax.axis_size(EXPERT)
    totals = exchange(jnp.broadcast_to(own, (experts, 1, 2)), EXPERT).sum(axis=(0, 1))
    norm_scale = lax.rsqrt(totals[0] / (totals[1] * d_whole * s) + 1e-06)

    inv, new_basis = factor(state, whole_gram, p, b)
    rotated = rotate(state, norm_scale.reshape(1), exchange(cross, ROW), inv, stale)
    return new_basis[None], rotated[None]


def solution(mesh):
    torus = Mesh(mesh.devices.reshape(16, 2, 4, 4), EXPERT + ROW)
    placed = (P(EXPERT, ROW, None), P(EXPERT, ROW, None), P(EXPERT), P(EXPERT))

    def whole(grads, basis, loads, flags):
        return jax.shard_map(
            functools.partial(on_device, grads.shape[1]),
            mesh=torus,
            in_specs=placed,
            out_specs=(P(EXPERT, ROW, None), P(EXPERT, None, ROW)),
            check_vma=False,
        )(grads, basis, loads, flags)

    return whole
```

```python
import functools

import jax
import jax.numpy as jnp
from jax import lax
from jax.experimental import pallas as pl
from jax.experimental.pallas import tpu as pltpu
from jax.sharding import Mesh
from jax.sharding import PartitionSpec as P

ROW = ("row_0", "row_1")
EXPERT = ("expert_0", "expert_1")
F32 = jnp.float32
BF16 = jnp.bfloat16
HIGH = lax.Precision.HIGHEST
BLOCK = 32
STAGGER = 9000
NT = (((1,), (1,)), ((), ()))
TN = (((0,), (0,)), ((), ()))
VM = pl.BlockSpec(memory_space=pltpu.VMEM)
SM = pl.BlockSpec(memory_space=pltpu.SMEM)
HBM = pl.BlockSpec(memory_space=pltpu.HBM)


def cost(flops, nbytes):
    return pl.CostEstimate(flops=int(flops), bytes_accessed=int(nbytes), transcendentals=0)


def params():
    return pltpu.CompilerParams(vmem_limit_bytes=16 * 1024 * 1024)


def product_columns(lt, g_ref, i):
    return jnp.dot(lt, g_ref[:, 256 * i : 256 * (i + 1)], preferred_element_type=F32)


def put(both, held_ref, out_ref, sem, i):
    k = both.shape[0]
    for h in range(2):
        held_ref[2 * i + h] = both[:, 128 * h : 128 * (h + 1)]
    copy = pltpu.make_async_copy(
        held_ref.at[pl.ds(2 * i, 2)], out_ref.at[pl.ds(2 * i, 2), pl.ds(0, k), :], sem.at[i]
    )
    copy.start()
    return copy


def first_kernel(state_ref, left_hbm, g_hbm, out_ref, left_ref, g_ref, held_ref, extra_ref, in_sem, out_sem):
    n, k, _ = held_ref.shape
    pairs = n // 2
    left_copy = pltpu.make_async_copy(left_hbm, left_ref, in_sem.at[pairs])
    left_copy.start()
    loads = []
    for i in range(pairs):
        cols = pl.ds(256 * i, 256)
        loads.append(pltpu.make_async_copy(g_hbm.at[:, cols], g_ref.at[:, cols], in_sem.at[i]))
        loads[-1].start()

    @pl.when(state_ref[2] > 0)
    def _():
        pl.delay(STAGGER)

    left_copy.wait()
    lt = left_ref[...].astype(F32).T.astype(BF16)
    squares = jnp.zeros((8, 256), F32)
    stores = []
    for i in range(pairs):
        loads[i].wait()
        stores.append(put(product_columns(lt, g_ref, i), held_ref, out_ref, out_sem, i))
        part = g_ref[:, 256 * i : 256 * (i + 1)].astype(F32)
        squares = squares + (part * part).reshape(-1, 8, 256).sum(axis=0)
    live = state_ref[1] > 0
    squares = jnp.where(live, squares[:, :128] + squares[:, 128:], 0.0)
    slot = jnp.where(live, jnp.full((8, 128), 1.0 / (8 * 128 * n), F32), 0.0)
    for j in range(n):
        extra_ref[j, :8, :] = squares
        extra_ref[j, 8:, :] = slot
    last = pltpu.make_async_copy(extra_ref, out_ref.at[:, pl.ds(k, 16), :], out_sem.at[pairs])
    last.start()
    for copy in stores:
        copy.wait()
    last.wait()


def first(state, left, g):
    d, k = left.shape
    s = g.shape[1]
    n = s // 128
    return pl.pallas_call(
        first_kernel,
        in_specs=[SM, HBM, HBM],
        out_specs=HBM,
        out_shape=pltpu.HBM((n, k + 16, 128), F32),
        scratch_shapes=[
            pltpu.VMEM((d, k), BF16),
            pltpu.VMEM((d, s), BF16),
            pltpu.VMEM((n, k, 128), F32),
            pltpu.VMEM((n, 16, 128), F32),
            pltpu.SemaphoreType.DMA((n // 2 + 1,)),
            pltpu.SemaphoreType.DMA((n // 2 + 1,)),
        ],
        compiler_params=params(),
        cost_estimate=cost(2 * d * k * s, 2 * d * (s + k) + 4 * k * s),
        name="first",
    )(state, pltpu.with_memory_space_constraint(left, pltpu.HBM), pltpu.with_memory_space_constraint(g, pltpu.HBM))


def second_kernel(left_ref, g_ref, out_ref, held_ref, sem):
    lt = left_ref[...].astype(F32).T.astype(BF16)
    n = held_ref.shape[0]
    stores = [put(product_columns(lt, g_ref, i), held_ref, out_ref, sem, i) for i in range(n // 2)]
    for copy in stores:
        copy.wait()


def second(left, g):
    d, k = left.shape
    s = g.shape[1]
    n = s // 128
    return pl.pallas_call(
        second_kernel,
        in_specs=[VM, VM],
        out_specs=HBM,
        out_shape=pltpu.HBM((n, k, 128), F32),
        scratch_shapes=[pltpu.VMEM((n, k, 128), F32), pltpu.SemaphoreType.DMA((n // 2,))],
        compiler_params=params(),
        cost_estimate=cost(2 * d * k * s, 2 * d * (s + k) + 4 * k * s),
        name="second",
    )(left, g)


def spread_kernel(kept, in_ref, own_ref, out_ref, sem):
    n = in_ref.shape[0]
    rows = out_ref.shape[1]
    step = rows // (1 if rows < 64 else 4)
    copies = []
    for c in range(rows // step):
        at = pl.ds(c * step, step)
        own_ref[at, :] = in_ref[:, at, :].sum(axis=0)
        for j in range(n):
            copies.append(pltpu.make_async_copy(own_ref.at[at], out_ref.at[j, at], sem.at[c, j]))
            copies[-1].start()
    if kept:
        own_ref[rows:, :] = in_ref[:, rows:, :].sum(axis=0)
    for copy in copies:
        copy.wait()


def spread(parts, kept):
    n, r, c = parts.shape
    return pl.pallas_call(
        functools.partial(spread_kernel, kept),
        in_specs=[VM],
        out_specs=[VM, HBM],
        out_shape=[jax.ShapeDtypeStruct((r, c), F32), pltpu.HBM((n, r - kept, c), F32)],
        scratch_shapes=[pltpu.SemaphoreType.DMA((4, n))],
        compiler_params=params(),
        cost_estimate=cost(n * r * c, 8 * n * r * c),
        name="spread",
    )(parts)


def power_of_two(m):
    s = jnp.ones_like(m)
    for e in (64, 32, 16, 8, 4, 2, 1):
        big = m >= 2.0**e
        s = jnp.where(big, s * 2.0**-e, s)
        m = jnp.where(big, m * 2.0**-e, m)
    for e in (64, 32, 16, 8, 4, 2, 1):
        small = m < 2.0 ** (1 - e)
        s = jnp.where(small, s * 2.0 ** (e - 1), s)
        m = jnp.where(small, m * 2.0 ** (e - 1), m)
    return s


def power_kernel(g_ref, w_ref, extra_ref, p_ref, gram_ref):
    n = w_ref.shape[0]
    k = p_ref.shape[1]
    m = jnp.abs(w_ref[0])
    for j in range(1, n):
        m = jnp.maximum(m, jnp.abs(w_ref[j]))
    scale = power_of_two(jnp.max(m, axis=1, keepdims=True))
    acc = jnp.zeros(p_ref.shape, F32)
    for j in range(0, n, 2):
        w = jnp.concatenate([w_ref[j], w_ref[j + 1]], axis=1)
        w = (w * scale).astype(BF16)
        acc = acc + lax.dot_general(g_ref[:, 128 * j : 128 * j + 256], w, NT, preferred_element_type=F32)
    p = acc.astype(BF16)
    p_ref[...] = p
    pt = p.astype(F32).T.astype(BF16)
    gram = jnp.dot(pt, p, preferred_element_type=F32)
    gram_ref[:, : k // n, :] = gram.reshape(n, k // n, k)
    extra = jnp.concatenate([extra_ref[:8, :], extra_ref[8:, :]], axis=1)
    for j in range(n):
        gram_ref[j, k // n :, :] = extra


def power(g, w, extra):
    d, s = g.shape
    n, k, _ = w.shape
    return pl.pallas_call(
        power_kernel,
        in_specs=[VM, VM, VM],
        out_specs=[VM, VM],
        out_shape=[jax.ShapeDtypeStruct((d, k), BF16), jax.ShapeDtypeStruct((n, k // n + 8, k), F32)],
        compiler_params=params(),
        cost_estimate=cost(2 * d * k * s, 2 * d * s + 4 * k * s),
        name="power",
    )(g, w, extra)


def sub(v, r):
    return jnp.broadcast_to(v[r : r + 1, :], v.shape)


def small_inverse(d):
    groups = BLOCK // 8
    row = lax.broadcasted_iota(jnp.int32, (8, 128), 0)
    lane = lax.broadcasted_iota(jnp.int32, (8, 128), 1)
    x = [jnp.where(lane == row + 8 * g, 1.0, 0.0) for g in range(groups)]
    c = [
        {g: jnp.broadcast_to(d[8 * g : 8 * g + 8, k : k + 1], (8, 128)) for g in range(k // 8, groups)}
        for k in range(BLOCK)
    ]
    for j in range(BLOCK):
        gj, sj = j // 8, j % 8
        r = lax.rsqrt(sub(c[j][gj], sj))
        low = {g: c[j][g] * r for g in range(gj, groups)}
        for k in range(j + 1, BLOCK):
            at = sub(low[k // 8], k % 8)
            for g in range(k // 8, groups):
                c[k][g] = c[k][g] - low[g] * at
        xr = sub(x[gj], sj) * r
        below = jnp.where(row > sj, low[gj], 0.0)
        x[gj] = jnp.where(row == sj, xr, x[gj] - below * xr)
        for g in range(gj + 1, groups):
            x[g] = x[g] - low[g] * xr
    return jnp.concatenate(x, axis=0)


def factor_kernel(refresh_ref, a_ref, p_ref, basis_ref, inv_ref, new_ref, t_ref):
    k = inv_ref.shape[0]
    a = a_ref[...].reshape(k, k)
    lane = lax.broadcasted_iota(jnp.int32, (BLOCK, k), 1)
    row = lax.broadcasted_iota(jnp.int32, (BLOCK, k), 0)
    for b in range(k // BLOCK):
        lo = b * BLOCK
        hi = lo + BLOCK
        r = jnp.where(lane >= lo, a[lo:hi, :], 0.0)
        if b:
            t = t_ref[:lo, :]
            at_lane = lax.broadcasted_iota(jnp.int32, (lo, k), 1)
            at_row = lax.broadcasted_iota(jnp.int32, (lo, k), 0)
            tm = jnp.where(jnp.logical_and(at_lane < lo, at_row < at_lane), 0.0, t)
            r = r - lax.dot_general(t[:, lo:hi], tm, TN, precision=HIGH, preferred_element_type=F32)
        x = small_inverse(r[:, lo:hi])[:, :BLOCK]
        inside = jnp.logical_and(lane >= lo, lane < hi)
        r = jnp.where(inside, jnp.where(lane - lo == row, 1.0, 0.0), r)
        t_ref[lo:hi, :] = jnp.dot(x, r, precision=HIGH, preferred_element_type=F32)
    whole_lane = lax.broadcasted_iota(jnp.int32, (k, k), 1)
    whole_row = lax.broadcasted_iota(jnp.int32, (k, k), 0)
    inv = jnp.where(whole_lane <= whole_row, t_ref[...], 0.0)
    inv_ref[...] = inv
    fresh = lax.dot_general(p_ref[...].astype(F32), inv, NT, precision=HIGH, preferred_element_type=F32)
    old = jnp.where(refresh_ref[1] > 0, basis_ref[...].astype(F32), 0.0)
    new_ref[...] = jnp.where(refresh_ref[0] > 0, fresh, old)


def factor(state, gram, p, basis):
    d, k = p.shape
    return pl.pallas_call(
        factor_kernel,
        in_specs=[SM, VM, VM, VM],
        out_specs=[VM, VM],
        out_shape=[jax.ShapeDtypeStruct((k, k), F32), jax.ShapeDtypeStruct((d, k), F32)],
        scratch_shapes=[pltpu.VMEM((k, k), F32)],
        compiler_params=params(),
        cost_estimate=cost(6e9, 4 * d * k),
        name="factor",
    )(state, gram, p, basis)


def rotate_kernel(size, state_ref, sums_ref, parts_ref, inv_ref, stale_ref, out_ref):
    fresh = jnp.dot(inv_ref[...], parts_ref[...].sum(axis=0), precision=HIGH, preferred_element_type=F32)
    squares = jnp.sum(sums_ref[:, :128], axis=(0, 1), keepdims=True)
    slots = jnp.sum(sums_ref[:, 128:], axis=(0, 1), keepdims=True)
    scale = lax.rsqrt(squares / (slots * size) + 1e-06)
    old = jnp.where(state_ref[1] > 0, stale_ref[...], 0.0)
    out_ref[...] = jnp.where(state_ref[0] > 0, fresh, old) * scale


def rotate(size, state, sums, parts, inv, stale):
    n, k, c = parts.shape
    return pl.pallas_call(
        functools.partial(rotate_kernel, size),
        in_specs=[SM, VM, VM, VM, VM],
        out_specs=VM,
        out_shape=jax.ShapeDtypeStruct((k, c), F32),
        compiler_params=params(),
        cost_estimate=cost(2 * k * k * c, 4 * n * k * c),
        name="rotate",
    )(state, sums, parts, inv, stale)


def exchange(blocks, axes):
    return lax.all_to_all(blocks, axes, split_axis=0, concat_axis=0, tiled=True)


def between_planes(value):
    far = lax.axis_size(EXPERT[0])
    rows = lax.axis_size(ROW)
    pairs = [(z * rows + r, (z + r) % far * rows + r) for z in range(far) for r in range(rows)]
    return lax.ppermute(value, (EXPERT[0],) + ROW, pairs)


def both_cores(value):
    return value + lax.ppermute(value, EXPERT[1], [(0, 1), (1, 0)])


def on_device(d_whole, grads, basis, loads, flags):
    g, b = grads[0], basis[0]
    k = b.shape[1]
    s = g.shape[1]
    live = loads[0] >= 1
    refresh = jnp.logical_and(live, flags[0] == 1)
    late = lax.axis_index(EXPERT[1]) == 0
    state = jnp.stack([refresh, live, late]).astype(jnp.int32)

    received = exchange(first(state, b, g), ROW)
    n = received.shape[0]
    own, copies = spread(received, 16)
    stale, plane = own[:k], own[k:]
    planes = between_planes(plane)
    received, planes = lax.optimization_barrier((exchange(copies, ROW), planes))
    p, gram = power(g, received, planes)
    own, gram_copies = spread(exchange(gram, ROW), 8)
    cross = second(p, g)
    whole_gram = exchange(gram_copies, ROW)
    inv, new_basis = factor(state, whole_gram, p, b)
    inv, core = lax.optimization_barrier((inv, own[k // n :]))
    rotated = rotate(float(d_whole * s), state, both_cores(core), exchange(cross, ROW), inv, stale)
    return new_basis[None], rotated[None]


def solution(mesh):
    torus = Mesh(mesh.devices.reshape(16, 2, 4, 4), EXPERT + ROW)
    placed = (P(EXPERT, ROW, None), P(EXPERT, ROW, None), P(EXPERT), P(EXPERT))

    def whole(grads, basis, loads, flags):
        return jax.shard_map(
            functools.partial(on_device, grads.shape[1]),
            mesh=torus,
            in_specs=placed,
            out_specs=(P(EXPERT, ROW, None), P(EXPERT, None, ROW)),
            check_vma=False,
        )(grads, basis, loads, flags)

    return whole
```

```python
import functools

import jax
import jax.numpy as jnp
from jax import lax
from jax.experimental import pallas as pl
from jax.experimental.pallas import tpu as pltpu
from jax.sharding import Mesh
from jax.sharding import PartitionSpec as P

ROW = ("row_0", "row_1")
EXPERT = ("expert_0", "expert_1")
F32 = jnp.float32
BF16 = jnp.bfloat16
HIGH = lax.Precision.HIGHEST
BLOCK = 32
STAGGER = 10000
NT = (((1,), (1,)), ((), ()))
TN = (((0,), (0,)), ((), ()))
VM = pl.BlockSpec(memory_space=pltpu.VMEM)
SM = pl.BlockSpec(memory_space=pltpu.SMEM)
HBM = pl.BlockSpec(memory_space=pltpu.HBM)


def cost(flops, nbytes):
    return pl.CostEstimate(flops=int(flops), bytes_accessed=int(nbytes), transcendentals=0)


def params():
    return pltpu.CompilerParams(vmem_limit_bytes=16 * 1024 * 1024)


def product_columns(lt, g_ref, i):
    return jnp.dot(lt, g_ref[:, 256 * i : 256 * (i + 1)], preferred_element_type=F32)


def put_half(both, held_ref, out_ref, sem, i, top):
    k = both.shape[0] // 2
    for h in range(2):
        block = both[:, 128 * h : 128 * (h + 1)]
        held_ref[2 * i + h, :, :128] = block[:k, :]
        held_ref[2 * i + h, :, 128:] = block[k:, :]
    copy = pltpu.make_async_copy(
        held_ref.at[pl.ds(2 * i, 2)], out_ref.at[pl.ds(2 * i, 2), pl.ds(top, k), :], sem.at[i]
    )
    copy.start()
    return copy


def first_kernel(state_ref, left_hbm, g_hbm, out_ref, left_ref, g_ref, sem):
    n = out_ref.shape[0]
    k = left_ref.shape[1]
    pairs = n // 2
    wide = pairs // 2
    left_copy = pltpu.make_async_copy(left_hbm, left_ref, sem.at[2])
    left_copy.start()
    loads = []
    for i in range(2):
        cols = pl.ds(256 * wide * i, 256 * wide)
        loads.append(pltpu.make_async_copy(g_hbm.at[:, cols], g_ref.at[:, cols], sem.at[i]))
        loads[-1].start()

    @pl.when(state_ref[2] > 0)
    def _():
        pl.delay(STAGGER)

    left_copy.wait()
    lt = left_ref[...].astype(F32).T.astype(BF16)
    squares = jnp.zeros((8, 256), F32)
    for i in range(pairs):
        if i % wide == 0:
            loads[i // wide].wait()
        both = product_columns(lt, g_ref, i)
        for h in range(2):
            out_ref[2 * i + h, :k, :] = both[:, 128 * h : 128 * (h + 1)]
        part = g_ref[:, 256 * i : 256 * (i + 1)].astype(F32)
        squares = squares + (part * part).reshape(-1, 8, 256).sum(axis=0)
    live = state_ref[1] > 0
    squares = jnp.where(live, squares[:, :128] + squares[:, 128:], 0.0)
    slot = jnp.where(live, jnp.full((8, 128), 1.0 / (8 * 128 * n), F32), 0.0)
    for j in range(n):
        out_ref[j, k : k + 8, :] = squares
        out_ref[j, k + 8 :, :] = slot


def first(state, left, g):
    d, k = left.shape
    s = g.shape[1]
    n = s // 128
    return pl.pallas_call(
        first_kernel,
        in_specs=[SM, HBM, HBM],
        out_specs=VM,
        out_shape=jax.ShapeDtypeStruct((n, k + 16, 128), F32),
        scratch_shapes=[pltpu.VMEM((d, k), BF16), pltpu.VMEM((d, s), BF16), pltpu.SemaphoreType.DMA((3,))],
        compiler_params=params(),
        cost_estimate=cost(2 * d * k * s, 2 * d * (s + k) + 4 * k * s),
        name="first",
    )(state, pltpu.with_memory_space_constraint(left, pltpu.HBM), pltpu.with_memory_space_constraint(g, pltpu.HBM))


def second_kernel(top, left_ref, g_ref, out_ref, held_ref, sem):
    lt = left_ref[...].astype(F32).T.astype(BF16)
    lt = lt[lt.shape[0] // 2 :, :]
    n = held_ref.shape[0]
    stores = [put_half(product_columns(lt, g_ref, i), held_ref, out_ref, sem, i, top) for i in range(n // 2)]
    for copy in stores:
        copy.wait()


def second(left, g):
    d, k = left.shape
    s = g.shape[1]
    n = s // 128
    top = k // n
    return pl.pallas_call(
        functools.partial(second_kernel, top),
        in_specs=[VM, VM],
        out_specs=HBM,
        out_shape=pltpu.HBM((n, top + k // 4, 256), F32),
        scratch_shapes=[pltpu.VMEM((n, k // 4, 256), F32), pltpu.SemaphoreType.DMA((n // 2,))],
        compiler_params=params(),
        cost_estimate=cost(d * k * s, 2 * d * (s + k) + 2 * k * s),
        name="second",
    )(left, g)


def share_kernel(top, in_ref, open_ref, sums_ref, half_ref, out_ref, own_ref, sem):
    n = in_ref.shape[0]
    own_ref[...] = in_ref[:, :top, :].sum(axis=0)
    copies = []
    for j in range(n):
        copies.append(pltpu.make_async_copy(own_ref, out_ref.at[j, pl.ds(0, top)], sem.at[j]))
        copies[-1].start()
    sums_ref[...] = in_ref[:, top : top + 8, :].sum(axis=0)
    half_ref[...] = in_ref[:, top + 8 :, :].sum(axis=0)
    for copy in copies:
        copy.wait()


def share(parts, opened, top):
    n, r, c = parts.shape
    return pl.pallas_call(
        functools.partial(share_kernel, top),
        in_specs=[VM, HBM],
        out_specs=[VM, VM, HBM],
        out_shape=[
            jax.ShapeDtypeStruct((8, c), F32),
            jax.ShapeDtypeStruct((r - top - 8, c), F32),
            pltpu.HBM(opened.shape, F32),
        ],
        scratch_shapes=[pltpu.VMEM((top, c), F32), pltpu.SemaphoreType.DMA((n,))],
        input_output_aliases={1: 2},
        compiler_params=params(),
        cost_estimate=cost(n * r * c, 4 * n * r * c),
        name="share",
    )(parts, opened)


def spread_kernel(in_ref, own_out, kept_ref, out_ref, own_ref, sem):
    n = in_ref.shape[0]
    rows = own_ref.shape[0]
    step = rows // 4
    copies = []
    for c in range(4):
        at = pl.ds(c * step, step)
        own_ref[at, :] = in_ref[:, at, :].sum(axis=0)
        for j in range(n):
            copies.append(pltpu.make_async_copy(own_ref.at[at], out_ref.at[j, at], sem.at[c, j]))
            copies[-1].start()
    copies.append(pltpu.make_async_copy(own_ref, own_out, sem.at[4, 0]))
    copies[-1].start()
    kept_ref[...] = in_ref[:, rows:, :].sum(axis=0)
    for copy in copies:
        copy.wait()


def spread(parts, kept):
    n, r, c = parts.shape
    return pl.pallas_call(
        spread_kernel,
        in_specs=[VM],
        out_specs=[HBM, VM, HBM],
        out_shape=[
            pltpu.HBM((r - kept, c), F32),
            jax.ShapeDtypeStruct((kept, c), F32),
            pltpu.HBM((n, r - kept, c), F32),
        ],
        scratch_shapes=[pltpu.VMEM((r - kept, c), F32), pltpu.SemaphoreType.DMA((5, n))],
        compiler_params=params(),
        cost_estimate=cost(n * r * c, 8 * n * r * c),
        name="spread",
    )(parts)


def power_of_two(m):
    s = jnp.ones_like(m)
    for e in (64, 32, 16, 8, 4, 2, 1):
        big = m >= 2.0**e
        s = jnp.where(big, s * 2.0**-e, s)
        m = jnp.where(big, m * 2.0**-e, m)
    for e in (64, 32, 16, 8, 4, 2, 1):
        small = m < 2.0 ** (1 - e)
        s = jnp.where(small, s * 2.0 ** (e - 1), s)
        m = jnp.where(small, m * 2.0 ** (e - 1), m)
    return s


def power_kernel(g_ref, w_hbm, extra_ref, p_ref, out_ref, w_ref, head_ref, held_ref, in_sem, sem):
    n, k, _ = w_ref.shape
    top = k // n
    step = n // 4
    loads = []
    for c in range(4):
        at = pl.ds(c * step, step)
        loads.append(pltpu.make_async_copy(w_hbm.at[at], w_ref.at[at], in_sem.at[c]))
        loads[-1].start()
    m = jnp.zeros(w_ref.shape[1:], F32)
    acc = jnp.zeros(p_ref.shape, F32)
    for j in range(0, n, 2):
        if j % step == 0:
            loads[j // step].wait()
        m = jnp.maximum(m, jnp.maximum(jnp.abs(w_ref[j]), jnp.abs(w_ref[j + 1])))
        w = jnp.concatenate([w_ref[j], w_ref[j + 1]], axis=1).astype(BF16)
        acc = acc + lax.dot_general(g_ref[:, 128 * j : 128 * j + 256], w, NT, preferred_element_type=F32)
    scale = power_of_two(jnp.max(m.T, axis=0, keepdims=True))
    acc = acc * scale
    p = acc.astype(BF16)
    p_ref[...] = p
    pt = p.astype(F32).T.astype(BF16)
    half = pt[: k // 2, :]
    stores = [
        put_half(product_columns(half, g_ref, i), held_ref, out_ref, sem, i, top + 8) for i in range(n // 2)
    ]
    head_ref[:, :top, :] = jnp.dot(pt, p, preferred_element_type=F32).reshape(n, top, k)
    extra = jnp.concatenate([extra_ref[:8, :], extra_ref[8:, :]], axis=1)
    for j in range(n):
        head_ref[j, top:, :] = extra
    last = pltpu.make_async_copy(head_ref, out_ref.at[:, pl.ds(0, top + 8), :], sem.at[n // 2])
    last.start()
    for copy in stores:
        copy.wait()
    last.wait()


def power(g, w, extra):
    d, s = g.shape
    n, k, _ = w.shape
    top = k // n + 8
    return pl.pallas_call(
        power_kernel,
        in_specs=[VM, HBM, VM],
        out_specs=[VM, HBM],
        out_shape=[jax.ShapeDtypeStruct((d, k), BF16), pltpu.HBM((n, top + k // 4, k), F32)],
        scratch_shapes=[
            pltpu.VMEM(w.shape, F32),
            pltpu.VMEM((n, top, k), F32),
            pltpu.VMEM((n, k // 4, k), F32),
            pltpu.SemaphoreType.DMA((4,)),
            pltpu.SemaphoreType.DMA((n // 2 + 1,)),
        ],
        compiler_params=params(),
        cost_estimate=cost(3 * d * k * s, 2 * d * s + 6 * k * s),
        name="power",
    )(g, pltpu.with_memory_space_constraint(w, pltpu.HBM), extra)


def sub(v, r):
    return jnp.broadcast_to(v[r : r + 1, :], v.shape)


def small_inverse(d):
    groups = BLOCK // 8
    row = lax.broadcasted_iota(jnp.int32, (8, 128), 0)
    lane = lax.broadcasted_iota(jnp.int32, (8, 128), 1)
    x = [jnp.where(lane == row + 8 * g, 1.0, 0.0) for g in range(groups)]
    c = [
        {g: jnp.broadcast_to(d[8 * g : 8 * g + 8, k : k + 1], (8, 128)) for g in range(k // 8, groups)}
        for k in range(BLOCK)
    ]
    for j in range(BLOCK):
        gj, sj = j // 8, j % 8
        r = lax.rsqrt(sub(c[j][gj], sj))
        low = {g: c[j][g] * r for g in range(gj, groups)}
        for k in range(j + 1, BLOCK):
            at = sub(low[k // 8], k % 8)
            for g in range(k // 8, groups):
                c[k][g] = c[k][g] - low[g] * at
        xr = sub(x[gj], sj) * r
        below = jnp.where(row > sj, low[gj], 0.0)
        x[gj] = jnp.where(row == sj, xr, x[gj] - below * xr)
        for g in range(gj + 1, groups):
            x[g] = x[g] - low[g] * xr
    return jnp.concatenate(x, axis=0)


def lower_inverse(m_ref):
    k = m_ref.shape[0]
    lane = lax.broadcasted_iota(jnp.int32, (BLOCK, k), 1)
    row = lax.broadcasted_iota(jnp.int32, (BLOCK, k), 0)
    for b in range(k // BLOCK):
        lo = b * BLOCK
        hi = lo + BLOCK
        r = m_ref[lo:hi, :]
        x = small_inverse(r[:, lo:hi])[:, :BLOCK]
        inside = jnp.logical_and(lane >= lo, lane < hi)
        r = jnp.where(inside, jnp.where(lane - lo == row, 1.0, 0.0), r)
        t = jnp.dot(x, r, precision=HIGH, preferred_element_type=F32)
        m_ref[lo:hi, :] = jnp.where(lane < hi, t, 0.0)
        for at, end in ((hi, min(hi + BLOCK, k)), (hi + BLOCK, k)):
            if at < end:
                old = m_ref[at:end, :]
                shape = old.shape
                column = lax.broadcasted_iota(jnp.int32, shape, 1)
                old = jnp.where(jnp.logical_and(column >= lo, column < hi), 0.0, old)
                m_ref[at:end, :] = old - lax.dot_general(
                    t[:, at:end], t, TN, precision=HIGH, preferred_element_type=F32
                )


def finish_kernel(size, state_ref, sums_ref, half_ref, parts_ref, stale_ref, p_ref, basis_ref, new_ref, out_ref, m_ref):
    n = parts_ref.shape[0]
    k = m_ref.shape[0]
    top = k // n
    m_ref[...] = parts_ref[:, :top, :].reshape(k, k)
    upper = half_ref[...]
    lower = parts_ref[:, top:, :].sum(axis=0)
    cross = jnp.concatenate([upper[:, :128], upper[:, 128:], lower[:, :128], lower[:, 128:]], axis=0)
    lower_inverse(m_ref)
    inv = m_ref[...]
    p = p_ref[...]
    fresh = jnp.zeros(new_ref.shape, F32)
    rest = inv
    for _ in range(3):
        piece = rest.astype(BF16)
        rest = rest - piece.astype(F32)
        fresh = fresh + lax.dot_general(p, piece, NT, preferred_element_type=F32)
    old = jnp.where(state_ref[1] > 0, basis_ref[...].astype(F32), 0.0)
    new_ref[...] = jnp.where(state_ref[0] > 0, fresh, old)
    turned = jnp.dot(inv, cross, precision=HIGH, preferred_element_type=F32)
    squares = jnp.sum(sums_ref[:, :128], axis=(0, 1), keepdims=True)
    slots = jnp.sum(sums_ref[:, 128:], axis=(0, 1), keepdims=True)
    scale = lax.rsqrt(squares / (slots * size) + 1e-06)
    stale = jnp.where(state_ref[1] > 0, stale_ref[...], 0.0)
    out_ref[...] = jnp.where(state_ref[0] > 0, turned, stale) * scale


def finish(size, state, sums, half, parts, stale, p, basis):
    d, k = p.shape
    return pl.pallas_call(
        functools.partial(finish_kernel, size),
        in_specs=[SM] + [VM] * 6,
        out_specs=[VM, VM],
        out_shape=[jax.ShapeDtypeStruct((d, k), F32), jax.ShapeDtypeStruct((k, 128), F32)],
        scratch_shapes=[pltpu.VMEM((k, k), F32)],
        compiler_params=params(),
        cost_estimate=cost(6e9, 4 * d * k),
        name="finish",
    )(state, sums, half, parts, stale, p, basis)


def exchange(blocks, axes):
    return lax.all_to_all(blocks, axes, split_axis=0, concat_axis=0, tiled=True)


def between_planes(value):
    far = lax.axis_size(EXPERT[0])
    rows = lax.axis_size(ROW)
    pairs = [(z * rows + r, (z + r) % far * rows + r) for z in range(far) for r in range(rows)]
    return lax.ppermute(value, (EXPERT[0],) + ROW, pairs)


def both_cores(value):
    return value + lax.ppermute(value, EXPERT[1], [(0, 1), (1, 0)])


def on_device(d_whole, grads, basis, loads, flags):
    g, b = grads[0], basis[0]
    k = b.shape[1]
    s = g.shape[1]
    live = loads[0] >= 1
    refresh = jnp.logical_and(live, flags[0] == 1)
    late = lax.axis_index(EXPERT[1]) == 0
    state = jnp.stack([refresh, live, late]).astype(jnp.int32)

    received = exchange(first(state, b, g), ROW)
    n = received.shape[0]
    stale, plane, copies = spread(received, 16)
    planes = between_planes(plane)
    received, planes = lax.optimization_barrier((exchange(copies, ROW), planes))
    p, sent = power(g, received, planes)
    top = k // n
    sums, half, sent = share(exchange(sent, ROW), second(p, g), top)
    received, sums = lax.optimization_barrier((exchange(sent, ROW), both_cores(sums)))
    new_basis, rotated = finish(float(d_whole * s), state, sums, half, received, stale, p, b)
    return new_basis[None], rotated[None]


def solution(mesh):
    torus = Mesh(mesh.devices.reshape(16, 2, 4, 4), EXPERT + ROW)
    placed = (P(EXPERT, ROW, None), P(EXPERT, ROW, None), P(EXPERT), P(EXPERT))

    def whole(grads, basis, loads, flags):
        return jax.shard_map(
            functools.partial(on_device, grads.shape[1]),
            mesh=torus,
            in_specs=placed,
            out_specs=(P(EXPERT, ROW, None), P(EXPERT, None, ROW)),
            check_vma=False,
        )(grads, basis, loads, flags)

    return whole
```

```python
import functools

import jax
import jax.numpy as jnp
from jax import lax
from jax.experimental import pallas as pl
from jax.experimental.pallas import tpu as pltpu
from jax.sharding import Mesh
from jax.sharding import PartitionSpec as P

ROW = ("row_0", "row_1")
EXPERT = ("expert_0", "expert_1")
F32 = jnp.float32
BF16 = jnp.bfloat16
HIGH = lax.Precision.HIGHEST
BLOCK = 32
STAGGER = 10000
NT = (((1,), (1,)), ((), ()))
TN = (((0,), (0,)), ((), ()))
VM = pl.BlockSpec(memory_space=pltpu.VMEM)
SM = pl.BlockSpec(memory_space=pltpu.SMEM)
HBM = pl.BlockSpec(memory_space=pltpu.HBM)


def cost(flops, nbytes):
    return pl.CostEstimate(flops=int(flops), bytes_accessed=int(nbytes), transcendentals=0)


def params():
    return pltpu.CompilerParams(vmem_limit_bytes=16 * 1024 * 1024)


def product_columns(lt, g_ref, i):
    return jnp.dot(lt, g_ref[:, 256 * i : 256 * (i + 1)], preferred_element_type=F32)


def put_half(both, out_ref, i, top):
    k = both.shape[0] // 2
    for h in range(2):
        block = both[:, 128 * h : 128 * (h + 1)]
        out_ref[2 * i + h, top : top + k, :128] = block[:k, :]
        out_ref[2 * i + h, top : top + k, 128:] = block[k:, :]


def first_kernel(state_ref, left_hbm, g_hbm, out_ref, left_ref, g_ref, sem):
    n = out_ref.shape[0]
    k = left_ref.shape[1]
    pairs = n // 2
    wide = pairs // 2
    left_copy = pltpu.make_async_copy(left_hbm, left_ref, sem.at[2])
    left_copy.start()
    loads = []
    for i in range(2):
        cols = pl.ds(256 * wide * i, 256 * wide)
        loads.append(pltpu.make_async_copy(g_hbm.at[:, cols], g_ref.at[:, cols], sem.at[i]))
        loads[-1].start()

    @pl.when(state_ref[2] > 0)
    def _():
        pl.delay(STAGGER)

    left_copy.wait()
    lt = left_ref[...].astype(F32).T.astype(BF16)
    squares = jnp.zeros((8, 256), F32)
    for i in range(pairs):
        if i % wide == 0:
            loads[i // wide].wait()
        both = product_columns(lt, g_ref, i)
        for h in range(2):
            out_ref[2 * i + h, :k, :] = both[:, 128 * h : 128 * (h + 1)]
        part = g_ref[:, 256 * i : 256 * (i + 1)].astype(F32)
        squares = squares + (part * part).reshape(-1, 8, 256).sum(axis=0)
    live = state_ref[1] > 0
    squares = squares[:, :128] + squares[:, 128:]
    squares = jnp.where(live, squares[:4, :] + squares[4:, :], 0.0)
    slot = jnp.where(live, jnp.full((4, 128), 1.0 / (4 * 128 * n), F32), 0.0)
    extra = jnp.concatenate([squares, slot], axis=0)
    for j in range(n):
        out_ref[j, k:, :] = extra


def first(state, left, g):
    d, k = left.shape
    s = g.shape[1]
    n = s // 128
    return pl.pallas_call(
        first_kernel,
        in_specs=[SM, HBM, HBM],
        out_specs=VM,
        out_shape=jax.ShapeDtypeStruct((n, k + 8, 128), F32),
        scratch_shapes=[pltpu.VMEM((d, k), BF16), pltpu.VMEM((d, s), BF16), pltpu.SemaphoreType.DMA((3,))],
        compiler_params=params(),
        cost_estimate=cost(2 * d * k * s, 2 * d * (s + k) + 4 * k * s),
        name="first",
    )(state, pltpu.with_memory_space_constraint(left, pltpu.HBM), pltpu.with_memory_space_constraint(g, pltpu.HBM))


def share_kernel(top, in_ref, rest_ref, sums_ref, half_ref, out_ref, own_ref, sem):
    n = in_ref.shape[0]
    copies = [pltpu.make_async_copy(rest_ref, out_ref.at[:, pl.ds(top, rest_ref.shape[1]), :], sem.at[n])]
    copies[-1].start()
    own_ref[...] = in_ref[:, :top, :].sum(axis=0)
    for j in range(n):
        copies.append(pltpu.make_async_copy(own_ref, out_ref.at[j, pl.ds(0, top)], sem.at[j]))
        copies[-1].start()
    sums_ref[...] = in_ref[:, top : top + 8, :128].sum(axis=0)
    half_ref[...] = in_ref[:, top + 8 :, :].sum(axis=0)
    for copy in copies:
        copy.wait()


def share(parts, rest, top):
    n, r, c = parts.shape
    below = rest.shape[1]
    return pl.pallas_call(
        functools.partial(share_kernel, top),
        in_specs=[VM, VM],
        out_specs=[VM, VM, HBM],
        out_shape=[
            jax.ShapeDtypeStruct((8, 128), F32),
            jax.ShapeDtypeStruct((r - top - 8, c), F32),
            pltpu.HBM((n, top + below, c), F32),
        ],
        scratch_shapes=[pltpu.VMEM((top, c), F32), pltpu.SemaphoreType.DMA((n + 1,))],
        compiler_params=params(),
        cost_estimate=cost(n * r * c, 4 * n * r * c),
        name="share",
    )(parts, rest)


def spread_kernel(in_ref, own_out, kept_ref, out_ref, own_ref, sem):
    n = in_ref.shape[0]
    rows = own_ref.shape[0]
    step = rows // 4
    copies = []
    for c in range(4):
        at = pl.ds(c * step, step)
        own_ref[at, :] = in_ref[:, at, :].sum(axis=0)
        for j in range(n):
            copies.append(pltpu.make_async_copy(own_ref.at[at], out_ref.at[j, at], sem.at[c, j]))
            copies[-1].start()
    copies.append(pltpu.make_async_copy(own_ref, own_out, sem.at[4, 0]))
    copies[-1].start()
    kept_ref[...] = in_ref[:, rows:, :].sum(axis=0)
    for copy in copies:
        copy.wait()


def spread(parts, kept):
    n, r, c = parts.shape
    return pl.pallas_call(
        spread_kernel,
        in_specs=[VM],
        out_specs=[HBM, VM, HBM],
        out_shape=[
            pltpu.HBM((r - kept, c), F32),
            jax.ShapeDtypeStruct((kept, c), F32),
            pltpu.HBM((n, r - kept, c), F32),
        ],
        scratch_shapes=[pltpu.VMEM((r - kept, c), F32), pltpu.SemaphoreType.DMA((5, n))],
        compiler_params=params(),
        cost_estimate=cost(n * r * c, 8 * n * r * c),
        name="spread",
    )(parts)


def power_of_two(m):
    s = jnp.ones_like(m)
    for e in (64, 32, 16, 8, 4, 2, 1):
        big = m >= 2.0**e
        s = jnp.where(big, s * 2.0**-e, s)
        m = jnp.where(big, m * 2.0**-e, m)
    for e in (64, 32, 16, 8, 4, 2, 1):
        small = m < 2.0 ** (1 - e)
        s = jnp.where(small, s * 2.0 ** (e - 1), s)
        m = jnp.where(small, m * 2.0 ** (e - 1), m)
    return s


def power_kernel(g_ref, w_hbm, extra_ref, p_ref, out_ref, rest_ref, w_ref, in_sem):
    n, k, _ = w_ref.shape
    top = k // n
    step = n // 4
    loads = []
    for c in range(4):
        at = pl.ds(c * step, step)
        loads.append(pltpu.make_async_copy(w_hbm.at[at], w_ref.at[at], in_sem.at[c]))
        loads[-1].start()
    m = jnp.zeros(w_ref.shape[1:], F32)
    acc = jnp.zeros(p_ref.shape, F32)
    for j in range(0, n, 2):
        if j % step == 0:
            loads[j // step].wait()
        m = jnp.maximum(m, jnp.maximum(jnp.abs(w_ref[j]), jnp.abs(w_ref[j + 1])))
        w = jnp.concatenate([w_ref[j], w_ref[j + 1]], axis=1).astype(BF16)
        acc = acc + lax.dot_general(g_ref[:, 128 * j : 128 * j + 256], w, NT, preferred_element_type=F32)
    scale = power_of_two(jnp.max(m.T, axis=0, keepdims=True))
    acc = acc * scale
    p = acc.astype(BF16)
    p_ref[...] = p
    pt = p.astype(F32).T.astype(BF16)
    out_ref[:, :top, :] = jnp.dot(pt, p, preferred_element_type=F32).reshape(n, top, k)
    extra = jnp.concatenate([extra_ref[...], jnp.zeros((8, k - 128), F32)], axis=1)
    for j in range(n):
        out_ref[j, top : top + 8, :] = extra
    for i in range(n // 2):
        both = product_columns(pt, g_ref, i)
        put_half(both[: k // 2, :], out_ref, i, top + 8)
        put_half(both[k // 2 :, :], rest_ref, i, 0)


def power(g, w, extra):
    d, s = g.shape
    n, k, _ = w.shape
    return pl.pallas_call(
        power_kernel,
        in_specs=[VM, HBM, VM],
        out_specs=[VM, VM, VM],
        out_shape=[
            jax.ShapeDtypeStruct((d, k), BF16),
            jax.ShapeDtypeStruct((n, k // n + 8 + k // 4, k), F32),
            jax.ShapeDtypeStruct((n, k // 4, k), F32),
        ],
        scratch_shapes=[pltpu.VMEM(w.shape, F32), pltpu.SemaphoreType.DMA((4,))],
        compiler_params=params(),
        cost_estimate=cost(4 * d * k * s, 2 * d * s + 8 * k * s),
        name="power",
    )(g, pltpu.with_memory_space_constraint(w, pltpu.HBM), extra)


def sub(v, r):
    return jnp.broadcast_to(v[r : r + 1, :], v.shape)


def small_inverse(d):
    groups = BLOCK // 8
    row = lax.broadcasted_iota(jnp.int32, (8, 128), 0)
    lane = lax.broadcasted_iota(jnp.int32, (8, 128), 1)
    x = [jnp.where(lane == row + 8 * g, 1.0, 0.0) for g in range(groups)]
    c = [
        {g: jnp.broadcast_to(d[8 * g : 8 * g + 8, k : k + 1], (8, 128)) for g in range(k // 8, groups)}
        for k in range(BLOCK)
    ]
    for j in range(BLOCK):
        gj, sj = j // 8, j % 8
        r = lax.rsqrt(sub(c[j][gj], sj))
        low = {g: c[j][g] * r for g in range(gj, groups)}
        for k in range(j + 1, BLOCK):
            at = sub(low[k // 8], k % 8)
            for g in range(k // 8, groups):
                c[k][g] = c[k][g] - low[g] * at
        xr = sub(x[gj], sj) * r
        below = jnp.where(row > sj, low[gj], 0.0)
        x[gj] = jnp.where(row == sj, xr, x[gj] - below * xr)
        for g in range(gj + 1, groups):
            x[g] = x[g] - low[g] * xr
    return jnp.concatenate(x, axis=0)


def lower_inverse(m_ref):
    k = m_ref.shape[0]
    lane = lax.broadcasted_iota(jnp.int32, (BLOCK, k), 1)
    row = lax.broadcasted_iota(jnp.int32, (BLOCK, k), 0)
    for b in range(k // BLOCK):
        lo = b * BLOCK
        hi = lo + BLOCK
        r = m_ref[lo:hi, :]
        x = small_inverse(r[:, lo:hi])[:, :BLOCK]
        inside = jnp.logical_and(lane >= lo, lane < hi)
        r = jnp.where(inside, jnp.where(lane - lo == row, 1.0, 0.0), r)
        t = jnp.dot(x, r, precision=HIGH, preferred_element_type=F32)
        m_ref[lo:hi, :] = jnp.where(lane < hi, t, 0.0)
        for at, end in ((hi, min(hi + BLOCK, k)), (hi + BLOCK, k)):
            if at < end:
                old = m_ref[at:end, :]
                shape = old.shape
                column = lax.broadcasted_iota(jnp.int32, shape, 1)
                old = jnp.where(jnp.logical_and(column >= lo, column < hi), 0.0, old)
                m_ref[at:end, :] = old - lax.dot_general(
                    t[:, at:end], t, TN, precision=HIGH, preferred_element_type=F32
                )


def finish_kernel(size, state_ref, sums_ref, half_ref, parts_ref, stale_ref, p_ref, basis_ref, new_ref, out_ref, m_ref):
    n = parts_ref.shape[0]
    k = m_ref.shape[0]
    top = k // n
    m_ref[...] = parts_ref[:, :top, :].reshape(k, k)
    upper = half_ref[...]
    lower = parts_ref[:, top:, :].sum(axis=0)
    cross = jnp.concatenate([upper[:, :128], upper[:, 128:], lower[:, :128], lower[:, 128:]], axis=0)
    lower_inverse(m_ref)
    inv = m_ref[...]
    p = p_ref[...]
    fresh = jnp.zeros(new_ref.shape, F32)
    rest = inv
    for _ in range(3):
        piece = rest.astype(BF16)
        rest = rest - piece.astype(F32)
        fresh = fresh + lax.dot_general(p, piece, NT, preferred_element_type=F32)
    old = jnp.where(state_ref[1] > 0, basis_ref[...].astype(F32), 0.0)
    new_ref[...] = jnp.where(state_ref[0] > 0, fresh, old)
    turned = jnp.dot(inv, cross, precision=HIGH, preferred_element_type=F32)
    squares = jnp.sum(sums_ref[:4, :], axis=(0, 1), keepdims=True)
    slots = jnp.sum(sums_ref[4:, :], axis=(0, 1), keepdims=True)
    scale = lax.rsqrt(squares / (slots * size) + 1e-06)
    stale = jnp.where(state_ref[1] > 0, stale_ref[...], 0.0)
    out_ref[...] = jnp.where(state_ref[0] > 0, turned, stale) * scale


def finish(size, state, sums, half, parts, stale, p, basis):
    d, k = p.shape
    return pl.pallas_call(
        functools.partial(finish_kernel, size),
        in_specs=[SM] + [VM] * 6,
        out_specs=[VM, VM],
        out_shape=[jax.ShapeDtypeStruct((d, k), F32), jax.ShapeDtypeStruct((k, 128), F32)],
        scratch_shapes=[pltpu.VMEM((k, k), F32)],
        compiler_params=params(),
        cost_estimate=cost(6e9, 4 * d * k),
        name="finish",
    )(state, sums, half, parts, stale, p, basis)


def exchange(blocks, axes):
    return lax.all_to_all(blocks, axes, split_axis=0, concat_axis=0, tiled=True)


def between_planes(value):
    far = lax.axis_size(EXPERT[0])
    rows = lax.axis_size(ROW)
    pairs = [(z * rows + r, (z + r) % far * rows + r) for z in range(far) for r in range(rows)]
    return lax.ppermute(value, (EXPERT[0],) + ROW, pairs)


def both_cores(value):
    return value + lax.ppermute(value, EXPERT[1], [(0, 1), (1, 0)])


def on_device(d_whole, grads, basis, loads, flags):
    g, b = grads[0], basis[0]
    k = b.shape[1]
    s = g.shape[1]
    live = loads[0] >= 1
    refresh = jnp.logical_and(live, flags[0] == 1)
    late = lax.axis_index(EXPERT[1]) == 0
    state = jnp.stack([refresh, live, late]).astype(jnp.int32)

    received = exchange(first(state, b, g), ROW)
    n = received.shape[0]
    stale, plane, copies = spread(received, 8)
    planes = between_planes(plane)
    received, planes = lax.optimization_barrier((exchange(copies, ROW), planes))
    p, sent, rest = power(g, received, planes)
    top = k // n
    sums, half, sent = share(exchange(sent, ROW), rest, top)
    received, sums = lax.optimization_barrier((exchange(sent, ROW), both_cores(sums)))
    new_basis, rotated = finish(float(d_whole * s), state, sums, half, received, stale, p, b)
    return new_basis[None], rotated[None]


def solution(mesh):
    torus = Mesh(mesh.devices.reshape(16, 2, 4, 4), EXPERT + ROW)
    placed = (P(EXPERT, ROW, None), P(EXPERT, ROW, None), P(EXPERT), P(EXPERT))

    def whole(grads, basis, loads, flags):
        return jax.shard_map(
            functools.partial(on_device, grads.shape[1]),
            mesh=torus,
            in_specs=placed,
            out_specs=(P(EXPERT, ROW, None), P(EXPERT, None, ROW)),
            check_vma=False,
        )(grads, basis, loads, flags)

    return whole
```

```python
import functools

import jax
import jax.numpy as jnp
from jax import lax
from jax.experimental import pallas as pl
from jax.experimental.pallas import tpu as pltpu
from jax.sharding import Mesh
from jax.sharding import PartitionSpec as P

ROW = ("row_0", "row_1")
EXPERT = ("expert_0", "expert_1")
F32 = jnp.float32
BF16 = jnp.bfloat16
HIGH = lax.Precision.HIGHEST
BLOCK = 32
STAGGER = 10000
NT = (((1,), (1,)), ((), ()))
TN = (((0,), (0,)), ((), ()))
VM = pl.BlockSpec(memory_space=pltpu.VMEM)
SM = pl.BlockSpec(memory_space=pltpu.SMEM)
HBM = pl.BlockSpec(memory_space=pltpu.HBM)


def cost(flops, nbytes):
    return pl.CostEstimate(flops=int(flops), bytes_accessed=int(nbytes), transcendentals=0)


def params():
    return pltpu.CompilerParams(vmem_limit_bytes=16 * 1024 * 1024)


def product_columns(lt, g_ref, i):
    return jnp.dot(lt, g_ref[:, 256 * i : 256 * (i + 1)], preferred_element_type=F32)


def put_half(both, out_ref, i, top):
    k = both.shape[0] // 2
    for h in range(2):
        block = both[:, 128 * h : 128 * (h + 1)]
        out_ref[2 * i + h, top : top + k, :128] = block[:k, :]
        out_ref[2 * i + h, top : top + k, 128:] = block[k:, :]


def first_kernel(state_ref, left_hbm, g_hbm, out_ref, left_ref, g_ref, sem):
    n = out_ref.shape[0]
    k = left_ref.shape[1]
    pairs = n // 2
    wide = pairs // 2
    left_copy = pltpu.make_async_copy(left_hbm, left_ref, sem.at[2])
    left_copy.start()
    loads = []
    for i in range(2):
        cols = pl.ds(256 * wide * i, 256 * wide)
        loads.append(pltpu.make_async_copy(g_hbm.at[:, cols], g_ref.at[:, cols], sem.at[i]))
        loads[-1].start()

    @pl.when(state_ref[2] > 0)
    def _():
        pl.delay(STAGGER)

    left_copy.wait()
    lt = left_ref[...].astype(F32).T.astype(BF16)
    squares = jnp.zeros((8, 256), F32)
    for i in range(pairs):
        if i % wide == 0:
            loads[i // wide].wait()
        both = product_columns(lt, g_ref, i)
        for h in range(2):
            out_ref[2 * i + h, :k, :] = both[:, 128 * h : 128 * (h + 1)]
        part = g_ref[:, 256 * i : 256 * (i + 1)].astype(F32)
        squares = squares + (part * part).reshape(-1, 8, 256).sum(axis=0)
    live = state_ref[1] > 0
    squares = squares[:, :128] + squares[:, 128:]
    squares = jnp.where(live, squares[:4, :] + squares[4:, :], 0.0)
    slot = jnp.where(live, jnp.full((4, 128), 1.0 / (4 * 128 * n), F32), 0.0)
    extra = jnp.concatenate([squares, slot], axis=0)
    for j in range(n):
        out_ref[j, k:, :] = extra


def first(state, left, g):
    d, k = left.shape
    s = g.shape[1]
    n = s // 128
    return pl.pallas_call(
        first_kernel,
        in_specs=[SM, HBM, HBM],
        out_specs=VM,
        out_shape=jax.ShapeDtypeStruct((n, k + 8, 128), F32),
        scratch_shapes=[pltpu.VMEM((d, k), BF16), pltpu.VMEM((d, s), BF16), pltpu.SemaphoreType.DMA((3,))],
        compiler_params=params(),
        cost_estimate=cost(2 * d * k * s, 2 * d * (s + k) + 4 * k * s),
        name="first",
    )(state, pltpu.with_memory_space_constraint(left, pltpu.HBM), pltpu.with_memory_space_constraint(g, pltpu.HBM))


def share_kernel(top, in_ref, rest_ref, sums_ref, half_ref, out_ref, wide_ref, sem):
    copies = [pltpu.make_async_copy(rest_ref, out_ref.at[:, pl.ds(top, rest_ref.shape[1]), :], sem.at[1])]
    copies[-1].start()
    total = in_ref[:, :top, :].sum(axis=0)
    wide_ref[...] = jnp.broadcast_to(total[None], wide_ref.shape)
    copies.append(pltpu.make_async_copy(wide_ref, out_ref.at[:, pl.ds(0, top), :], sem.at[0]))
    copies[-1].start()
    sums_ref[...] = in_ref[:, top : top + 8, :128].sum(axis=0)
    half_ref[...] = in_ref[:, top + 8 :, :].sum(axis=0)
    for copy in copies:
        copy.wait()


def share(parts, rest, top):
    n, r, c = parts.shape
    below = rest.shape[1]
    return pl.pallas_call(
        functools.partial(share_kernel, top),
        in_specs=[VM, VM],
        out_specs=[VM, VM, HBM],
        out_shape=[
            jax.ShapeDtypeStruct((8, 128), F32),
            jax.ShapeDtypeStruct((r - top - 8, c), F32),
            pltpu.HBM((n, top + below, c), F32),
        ],
        scratch_shapes=[pltpu.VMEM((n, top, c), F32), pltpu.SemaphoreType.DMA((2,))],
        compiler_params=params(),
        cost_estimate=cost(n * r * c, 4 * n * r * c),
        name="share",
    )(parts, rest)


def spread_kernel(in_ref, own_out, kept_ref, out_ref, own_ref, wide_ref, sem):
    rows = own_ref.shape[0]
    step = rows // 4
    copies = []
    for c in range(4):
        at = pl.ds(c * step, step)
        total = in_ref[:, at, :].sum(axis=0)
        own_ref[at, :] = total
        wide_ref[:, at, :] = jnp.broadcast_to(total[None], (wide_ref.shape[0], *total.shape))
        copies.append(pltpu.make_async_copy(wide_ref.at[:, at], out_ref.at[:, at], sem.at[c]))
        copies[-1].start()
    copies.append(pltpu.make_async_copy(own_ref, own_out, sem.at[4]))
    copies[-1].start()
    kept_ref[...] = in_ref[:, rows:, :].sum(axis=0)
    for copy in copies:
        copy.wait()


def spread(parts, kept):
    n, r, c = parts.shape
    return pl.pallas_call(
        spread_kernel,
        in_specs=[VM],
        out_specs=[HBM, VM, HBM],
        out_shape=[
            pltpu.HBM((r - kept, c), F32),
            jax.ShapeDtypeStruct((kept, c), F32),
            pltpu.HBM((n, r - kept, c), F32),
        ],
        scratch_shapes=[
            pltpu.VMEM((r - kept, c), F32),
            pltpu.VMEM((n, r - kept, c), F32),
            pltpu.SemaphoreType.DMA((5,)),
        ],
        compiler_params=params(),
        cost_estimate=cost(n * r * c, 8 * n * r * c),
        name="spread",
    )(parts)


def power_of_two(m):
    s = jnp.ones_like(m)
    for e in (64, 32, 16, 8, 4, 2, 1):
        big = m >= 2.0**e
        s = jnp.where(big, s * 2.0**-e, s)
        m = jnp.where(big, m * 2.0**-e, m)
    for e in (64, 32, 16, 8, 4, 2, 1):
        small = m < 2.0 ** (1 - e)
        s = jnp.where(small, s * 2.0 ** (e - 1), s)
        m = jnp.where(small, m * 2.0 ** (e - 1), m)
    return s


def power_kernel(g_ref, w_hbm, extra_ref, p_ref, out_ref, rest_ref, w_ref, in_sem):
    n, k, _ = w_ref.shape
    top = k // n
    step = n // 4
    loads = []
    for c in range(4):
        at = pl.ds(c * step, step)
        loads.append(pltpu.make_async_copy(w_hbm.at[at], w_ref.at[at], in_sem.at[c]))
        loads[-1].start()
    m = jnp.zeros(w_ref.shape[1:], F32)
    acc = jnp.zeros(p_ref.shape, F32)
    for j in range(0, n, 2):
        if j % step == 0:
            loads[j // step].wait()
        m = jnp.maximum(m, jnp.maximum(jnp.abs(w_ref[j]), jnp.abs(w_ref[j + 1])))
        w = jnp.concatenate([w_ref[j], w_ref[j + 1]], axis=1).astype(BF16)
        acc = acc + lax.dot_general(g_ref[:, 128 * j : 128 * j + 256], w, NT, preferred_element_type=F32)
    scale = power_of_two(jnp.max(m.T, axis=0, keepdims=True))
    acc = acc * scale
    p = acc.astype(BF16)
    p_ref[...] = p
    pt = p.astype(F32).T.astype(BF16)
    out_ref[:, :top, :] = jnp.dot(pt, p, preferred_element_type=F32).reshape(n, top, k)
    extra = jnp.concatenate([extra_ref[...], jnp.zeros((8, k - 128), F32)], axis=1)
    for j in range(n):
        out_ref[j, top : top + 8, :] = extra
    for i in range(n // 2):
        both = product_columns(pt, g_ref, i)
        put_half(both[: k // 2, :], out_ref, i, top + 8)
        put_half(both[k // 2 :, :], rest_ref, i, 0)


def power(g, w, extra):
    d, s = g.shape
    n, k, _ = w.shape
    return pl.pallas_call(
        power_kernel,
        in_specs=[VM, HBM, VM],
        out_specs=[VM, VM, VM],
        out_shape=[
            jax.ShapeDtypeStruct((d, k), BF16),
            jax.ShapeDtypeStruct((n, k // n + 8 + k // 4, k), F32),
            jax.ShapeDtypeStruct((n, k // 4, k), F32),
        ],
        scratch_shapes=[pltpu.VMEM(w.shape, F32), pltpu.SemaphoreType.DMA((4,))],
        compiler_params=params(),
        cost_estimate=cost(4 * d * k * s, 2 * d * s + 8 * k * s),
        name="power",
    )(g, pltpu.with_memory_space_constraint(w, pltpu.HBM), extra)


def sub(v, r):
    return jnp.broadcast_to(v[r : r + 1, :], v.shape)


def small_inverse(d):
    groups = BLOCK // 8
    row = lax.broadcasted_iota(jnp.int32, (8, 128), 0)
    lane = lax.broadcasted_iota(jnp.int32, (8, 128), 1)
    x = [jnp.where(lane % BLOCK == row + 8 * g, 1.0, 0.0) for g in range(groups)]
    c = [
        {g: jnp.broadcast_to(d[8 * g : 8 * g + 8, k : k + 1], (8, 128)) for g in range(k // 8, groups)}
        for k in range(BLOCK)
    ]
    for j in range(BLOCK):
        gj, sj = j // 8, j % 8
        r = lax.rsqrt(sub(c[j][gj], sj))
        low = {g: c[j][g] * r for g in range(gj, groups)}
        for k in range(j + 1, BLOCK):
            at = sub(low[k // 8], k % 8)
            for g in range(k // 8, groups):
                c[k][g] = c[k][g] - low[g] * at
        xr = sub(x[gj], sj) * r
        below = jnp.where(row > sj, low[gj], 0.0)
        x[gj] = jnp.where(row == sj, xr, x[gj] - below * xr)
        for g in range(gj + 1, groups):
            x[g] = x[g] - low[g] * xr
    return jnp.concatenate(x, axis=0)


def pieces(x):
    high = x.astype(BF16)
    rest = x - high.astype(F32)
    mid = rest.astype(BF16)
    return high, mid, (rest - mid.astype(F32)).astype(BF16)


def stack(x, order):
    parts = pieces(x)
    return jnp.concatenate([parts[i] for i in order], axis=0)


LEFT = (0, 0, 1, 0, 2, 1)
RIGHT = (0, 1, 0, 2, 0, 1)


def beside(x):
    parts = [p.astype(F32) for p in pieces(x)]
    place = lax.broadcasted_iota(jnp.int32, x.shape, 1) // BLOCK
    per = 128 // BLOCK
    out = []
    for start in range(0, len(LEFT), per):
        wide = parts[LEFT[start]]
        for i, which in enumerate(LEFT[start : start + per]):
            wide = jnp.where(place == i, parts[which], wide)
        out.append(wide[:, : BLOCK * len(LEFT[start : start + per])])
    return jnp.concatenate(out, axis=1).astype(BF16)


def lower_inverse(m_ref):
    k = m_ref.shape[0]
    lane = lax.broadcasted_iota(jnp.int32, (BLOCK, k), 1)
    row = lax.broadcasted_iota(jnp.int32, (BLOCK, k), 0)
    for b in range(k // BLOCK):
        lo = b * BLOCK
        hi = lo + BLOCK
        r = m_ref[lo:hi, :]
        x = small_inverse(r[:, lo:hi])
        inside = jnp.logical_and(lane >= lo, lane < hi)
        r = jnp.where(inside, jnp.where(lane - lo == row, 1.0, 0.0), r)
        t = jnp.dot(beside(x), stack(r, RIGHT), preferred_element_type=F32)
        m_ref[lo:hi, :] = jnp.where(lane < hi, t, 0.0)
        if hi < k:
            left, right = stack(t, LEFT), stack(t, RIGHT)
        for at, end in ((hi, min(hi + BLOCK, k)), (hi + BLOCK, k)):
            if at < end:
                old = m_ref[at:end, :]
                column = lax.broadcasted_iota(jnp.int32, old.shape, 1)
                old = jnp.where(jnp.logical_and(column >= lo, column < hi), 0.0, old)
                m_ref[at:end, :] = old - lax.dot_general(left[:, at:end], right, TN, preferred_element_type=F32)


def finish_kernel(size, state_ref, sums_ref, half_ref, parts_ref, stale_ref, p_ref, basis_ref, new_ref, out_ref, m_ref):
    n = parts_ref.shape[0]
    k = m_ref.shape[0]
    top = k // n
    m_ref[...] = parts_ref[:, :top, :].reshape(k, k)
    upper = half_ref[...]
    lower = parts_ref[:, top:, :].sum(axis=0)
    cross = jnp.concatenate([upper[:, :128], upper[:, 128:], lower[:, :128], lower[:, 128:]], axis=0)
    lower_inverse(m_ref)
    inv = m_ref[...]
    p = p_ref[...]
    fresh = jnp.zeros(new_ref.shape, F32)
    rest = inv
    for _ in range(3):
        piece = rest.astype(BF16)
        rest = rest - piece.astype(F32)
        fresh = fresh + lax.dot_general(p, piece, NT, preferred_element_type=F32)
    old = jnp.where(state_ref[1] > 0, basis_ref[...].astype(F32), 0.0)
    new_ref[...] = jnp.where(state_ref[0] > 0, fresh, old)
    turned = jnp.dot(inv, cross, precision=HIGH, preferred_element_type=F32)
    squares = jnp.sum(sums_ref[:4, :], axis=(0, 1), keepdims=True)
    slots = jnp.sum(sums_ref[4:, :], axis=(0, 1), keepdims=True)
    scale = lax.rsqrt(squares / (slots * size) + 1e-06)
    stale = jnp.where(state_ref[1] > 0, stale_ref[...], 0.0)
    out_ref[...] = jnp.where(state_ref[0] > 0, turned, stale) * scale


def finish(size, state, sums, half, parts, stale, p, basis):
    d, k = p.shape
    return pl.pallas_call(
        functools.partial(finish_kernel, size),
        in_specs=[SM] + [VM] * 6,
        out_specs=[VM, VM],
        out_shape=[jax.ShapeDtypeStruct((d, k), F32), jax.ShapeDtypeStruct((k, 128), F32)],
        scratch_shapes=[pltpu.VMEM((k, k), F32)],
        compiler_params=params(),
        cost_estimate=cost(6e9, 4 * d * k),
        name="finish",
    )(state, sums, half, parts, stale, p, basis)


def exchange(blocks, axes):
    return lax.all_to_all(blocks, axes, split_axis=0, concat_axis=0, tiled=True)


def between_planes(value):
    far = lax.axis_size(EXPERT[0])
    rows = lax.axis_size(ROW)
    pairs = [(z * rows + r, (z + r) % far * rows + r) for z in range(far) for r in range(rows)]
    return lax.ppermute(value, (EXPERT[0],) + ROW, pairs)


def both_cores(value):
    return value + lax.ppermute(value, EXPERT[1], [(0, 1), (1, 0)])


def on_device(d_whole, grads, basis, loads, flags):
    g, b = grads[0], basis[0]
    k = b.shape[1]
    s = g.shape[1]
    live = loads[0] >= 1
    refresh = jnp.logical_and(live, flags[0] == 1)
    late = lax.axis_index(EXPERT[1]) == 0
    state = jnp.stack([refresh, live, late]).astype(jnp.int32)

    received = exchange(first(state, b, g), ROW)
    n = received.shape[0]
    stale, plane, copies = spread(received, 8)
    planes = between_planes(plane)
    received, planes = lax.optimization_barrier((exchange(copies, ROW), planes))
    p, sent, rest = power(g, received, planes)
    top = k // n
    sums, half, sent = share(exchange(sent, ROW), rest, top)
    received, sums = lax.optimization_barrier((exchange(sent, ROW), both_cores(sums)))
    new_basis, rotated = finish(float(d_whole * s), state, sums, half, received, stale, p, b)
    return new_basis[None], rotated[None]


def solution(mesh):
    torus = Mesh(mesh.devices.reshape(16, 2, 4, 4), EXPERT + ROW)
    placed = (P(EXPERT, ROW, None), P(EXPERT, ROW, None), P(EXPERT), P(EXPERT))

    def whole(grads, basis, loads, flags):
        return jax.shard_map(
            functools.partial(on_device, grads.shape[1]),
            mesh=torus,
            in_specs=placed,
            out_specs=(P(EXPERT, ROW, None), P(EXPERT, None, ROW)),
            check_vma=False,
        )(grads, basis, loads, flags)

    return whole
```

```python
import functools

import jax
import jax.numpy as jnp
from jax import lax
from jax.experimental import pallas as pl
from jax.experimental.pallas import tpu as pltpu
from jax.sharding import Mesh
from jax.sharding import PartitionSpec as P

ROW = ("row_0", "row_1")
EXPERT = ("expert_0", "expert_1")
F32 = jnp.float32
BF16 = jnp.bfloat16
HIGH = lax.Precision.HIGHEST
BLOCK = 32
STAGGER = 10000
NT = (((1,), (1,)), ((), ()))
TN = (((0,), (0,)), ((), ()))
VM = pl.BlockSpec(memory_space=pltpu.VMEM)
SM = pl.BlockSpec(memory_space=pltpu.SMEM)
HBM = pl.BlockSpec(memory_space=pltpu.HBM)


def cost(flops, nbytes):
    return pl.CostEstimate(flops=int(flops), bytes_accessed=int(nbytes), transcendentals=0)


def params():
    return pltpu.CompilerParams(vmem_limit_bytes=16 * 1024 * 1024)


def product_columns(lt, g_ref, i):
    return jnp.dot(lt, g_ref[:, 256 * i : 256 * (i + 1)], preferred_element_type=F32)


def put_half(both, out_ref, i, top):
    k = both.shape[0] // 2
    for h in range(2):
        block = both[:, 128 * h : 128 * (h + 1)]
        out_ref[2 * i + h, top : top + k, :128] = block[:k, :]
        out_ref[2 * i + h, top : top + k, 128:] = block[k:, :]


def first_kernel(loads_ref, left_hbm, g_hbm, out_ref, left_ref, g_ref, sem):
    n = out_ref.shape[0]
    k = left_ref.shape[1]
    pairs = n // 2
    wide = pairs // 2
    left_copy = pltpu.make_async_copy(left_hbm, left_ref, sem.at[2])
    left_copy.start()
    loads = []
    for i in range(2):
        cols = pl.ds(256 * wide * i, 256 * wide)
        loads.append(pltpu.make_async_copy(g_hbm.at[:, cols], g_ref.at[:, cols], sem.at[i]))
        loads[-1].start()

    @pl.when(lax.axis_index(EXPERT[1]) == 0)
    def _():
        pl.delay(STAGGER)

    left_copy.wait()
    lt = left_ref[...].astype(F32).T.astype(BF16)
    squares = jnp.zeros((8, 256), F32)
    for i in range(pairs):
        if i % wide == 0:
            loads[i // wide].wait()
        both = product_columns(lt, g_ref, i)
        for h in range(2):
            out_ref[2 * i + h, :k, :] = both[:, 128 * h : 128 * (h + 1)]
        part = g_ref[:, 256 * i : 256 * (i + 1)].astype(F32)
        squares = squares + (part * part).reshape(-1, 8, 256).sum(axis=0)
    live = loads_ref[0] >= 1
    squares = squares[:, :128] + squares[:, 128:]
    squares = jnp.where(live, squares[:4, :] + squares[4:, :], 0.0)
    slot = jnp.where(live, jnp.full((4, 128), 1.0 / (4 * 128 * n), F32), 0.0)
    extra = jnp.concatenate([squares, slot], axis=0)
    for j in range(n):
        out_ref[j, k:, :] = extra


def first(loads, left, g):
    d, k = left.shape
    s = g.shape[1]
    n = s // 128
    return pl.pallas_call(
        first_kernel,
        in_specs=[SM, HBM, HBM],
        out_specs=VM,
        out_shape=jax.ShapeDtypeStruct((n, k + 8, 128), F32),
        scratch_shapes=[pltpu.VMEM((d, k), BF16), pltpu.VMEM((d, s), BF16), pltpu.SemaphoreType.DMA((3,))],
        compiler_params=params(),
        cost_estimate=cost(2 * d * k * s, 2 * d * (s + k) + 4 * k * s),
        name="first",
    )(loads, pltpu.with_memory_space_constraint(left, pltpu.HBM), pltpu.with_memory_space_constraint(g, pltpu.HBM))


def share_kernel(top, in_ref, rest_ref, sums_ref, half_ref, out_ref, wide_ref, sem):
    copies = [pltpu.make_async_copy(rest_ref, out_ref.at[:, pl.ds(top, rest_ref.shape[1]), :], sem.at[1])]
    copies[-1].start()
    total = in_ref[:, :top, :].sum(axis=0)
    wide_ref[...] = jnp.broadcast_to(total[None], wide_ref.shape)
    copies.append(pltpu.make_async_copy(wide_ref, out_ref.at[:, pl.ds(0, top), :], sem.at[0]))
    copies[-1].start()
    sums_ref[...] = in_ref[:, top : top + 8, :128].sum(axis=0)
    half_ref[...] = in_ref[:, top + 8 :, :].sum(axis=0)
    for copy in copies:
        copy.wait()


def share(parts, rest, top):
    n, r, c = parts.shape
    below = rest.shape[1]
    return pl.pallas_call(
        functools.partial(share_kernel, top),
        in_specs=[VM, VM],
        out_specs=[VM, VM, HBM],
        out_shape=[
            jax.ShapeDtypeStruct((8, 128), F32),
            jax.ShapeDtypeStruct((r - top - 8, c), F32),
            pltpu.HBM((n, top + below, c), F32),
        ],
        scratch_shapes=[pltpu.VMEM((n, top, c), F32), pltpu.SemaphoreType.DMA((2,))],
        compiler_params=params(),
        cost_estimate=cost(n * r * c, 4 * n * r * c),
        name="share",
    )(parts, rest)


def spread_kernel(in_ref, own_out, kept_ref, out_ref, own_ref, wide_ref, sem):
    rows = own_ref.shape[0]
    step = rows // 4
    copies = []
    for c in range(4):
        at = pl.ds(c * step, step)
        total = in_ref[:, at, :].sum(axis=0)
        own_ref[at, :] = total
        wide_ref[:, at, :] = jnp.broadcast_to(total[None], (wide_ref.shape[0], *total.shape))
        copies.append(pltpu.make_async_copy(wide_ref.at[:, at], out_ref.at[:, at], sem.at[c]))
        copies[-1].start()
    copies.append(pltpu.make_async_copy(own_ref, own_out, sem.at[4]))
    copies[-1].start()
    kept_ref[...] = in_ref[:, rows:, :].sum(axis=0)
    for copy in copies:
        copy.wait()


def spread(parts, kept):
    n, r, c = parts.shape
    return pl.pallas_call(
        spread_kernel,
        in_specs=[VM],
        out_specs=[HBM, VM, HBM],
        out_shape=[
            pltpu.HBM((r - kept, c), F32),
            jax.ShapeDtypeStruct((kept, c), F32),
            pltpu.HBM((n, r - kept, c), F32),
        ],
        scratch_shapes=[
            pltpu.VMEM((r - kept, c), F32),
            pltpu.VMEM((n, r - kept, c), F32),
            pltpu.SemaphoreType.DMA((5,)),
        ],
        compiler_params=params(),
        cost_estimate=cost(n * r * c, 8 * n * r * c),
        name="spread",
    )(parts)


def power_of_two(m):
    s = jnp.ones_like(m)
    for e in (64, 32, 16, 8, 4, 2, 1):
        big = m >= 2.0**e
        s = jnp.where(big, s * 2.0**-e, s)
        m = jnp.where(big, m * 2.0**-e, m)
    for e in (64, 32, 16, 8, 4, 2, 1):
        small = m < 2.0 ** (1 - e)
        s = jnp.where(small, s * 2.0 ** (e - 1), s)
        m = jnp.where(small, m * 2.0 ** (e - 1), m)
    return s


def power_kernel(g_ref, w_hbm, extra_ref, p_ref, out_ref, rest_ref, w_ref, in_sem):
    n, k, _ = w_ref.shape
    top = k // n
    step = n // 4
    loads = []
    for c in range(4):
        at = pl.ds(c * step, step)
        loads.append(pltpu.make_async_copy(w_hbm.at[at], w_ref.at[at], in_sem.at[c]))
        loads[-1].start()
    m = jnp.zeros(w_ref.shape[1:], F32)
    acc = jnp.zeros(p_ref.shape, F32)
    for j in range(0, n, 2):
        if j % step == 0:
            loads[j // step].wait()
        m = jnp.maximum(m, jnp.maximum(jnp.abs(w_ref[j]), jnp.abs(w_ref[j + 1])))
        w = jnp.concatenate([w_ref[j], w_ref[j + 1]], axis=1).astype(BF16)
        acc = acc + lax.dot_general(g_ref[:, 128 * j : 128 * j + 256], w, NT, preferred_element_type=F32)
    scale = power_of_two(jnp.max(m.T, axis=0, keepdims=True))
    acc = acc * scale
    p = acc.astype(BF16)
    p_ref[...] = p
    pt = p.astype(F32).T.astype(BF16)
    out_ref[:, :top, :] = jnp.dot(pt, p, preferred_element_type=F32).reshape(n, top, k)
    extra = jnp.concatenate([extra_ref[...], jnp.zeros((8, k - 128), F32)], axis=1)
    for j in range(n):
        out_ref[j, top : top + 8, :] = extra
    for i in range(n // 2):
        both = product_columns(pt, g_ref, i)
        put_half(both[: k // 2, :], out_ref, i, top + 8)
        put_half(both[k // 2 :, :], rest_ref, i, 0)


def power(g, w, extra):
    d, s = g.shape
    n, k, _ = w.shape
    return pl.pallas_call(
        power_kernel,
        in_specs=[VM, HBM, VM],
        out_specs=[VM, VM, VM],
        out_shape=[
            jax.ShapeDtypeStruct((d, k), BF16),
            jax.ShapeDtypeStruct((n, k // n + 8 + k // 4, k), F32),
            jax.ShapeDtypeStruct((n, k // 4, k), F32),
        ],
        scratch_shapes=[pltpu.VMEM(w.shape, F32), pltpu.SemaphoreType.DMA((4,))],
        compiler_params=params(),
        cost_estimate=cost(4 * d * k * s, 2 * d * s + 8 * k * s),
        name="power",
    )(g, pltpu.with_memory_space_constraint(w, pltpu.HBM), extra)


def sub(v, r):
    return jnp.broadcast_to(v[r : r + 1, :], v.shape)


def small_inverse(d):
    groups = BLOCK // 8
    row = lax.broadcasted_iota(jnp.int32, (8, 128), 0)
    lane = lax.broadcasted_iota(jnp.int32, (8, 128), 1)
    x = [jnp.where(lane % BLOCK == row + 8 * g, 1.0, 0.0) for g in range(groups)]
    c = [
        {g: jnp.broadcast_to(d[8 * g : 8 * g + 8, k : k + 1], (8, 128)) for g in range(k // 8, groups)}
        for k in range(BLOCK)
    ]
    for j in range(BLOCK):
        gj, sj = j // 8, j % 8
        r = lax.rsqrt(sub(c[j][gj], sj))
        low = {g: c[j][g] * r for g in range(gj, groups)}
        for k in range(j + 1, BLOCK):
            at = sub(low[k // 8], k % 8)
            for g in range(k // 8, groups):
                c[k][g] = c[k][g] - low[g] * at
        xr = sub(x[gj], sj) * r
        below = jnp.where(row > sj, low[gj], 0.0)
        x[gj] = jnp.where(row == sj, xr, x[gj] - below * xr)
        for g in range(gj + 1, groups):
            x[g] = x[g] - low[g] * xr
    return jnp.concatenate(x, axis=0)


def pieces(x):
    high = x.astype(BF16)
    rest = x - high.astype(F32)
    mid = rest.astype(BF16)
    return high, mid, (rest - mid.astype(F32)).astype(BF16)


def stack(x, order):
    parts = pieces(x)
    return jnp.concatenate([parts[i] for i in order], axis=0)


LEFT = (0, 0, 1, 0, 2, 1)
RIGHT = (0, 1, 0, 2, 0, 1)


def beside(x):
    parts = [p.astype(F32) for p in pieces(x)]
    place = lax.broadcasted_iota(jnp.int32, x.shape, 1) // BLOCK
    per = 128 // BLOCK
    out = []
    for start in range(0, len(LEFT), per):
        wide = parts[LEFT[start]]
        for i, which in enumerate(LEFT[start : start + per]):
            wide = jnp.where(place == i, parts[which], wide)
        out.append(wide[:, : BLOCK * len(LEFT[start : start + per])])
    return jnp.concatenate(out, axis=1).astype(BF16)


def lower_inverse(m_ref):
    k = m_ref.shape[0]
    lane = lax.broadcasted_iota(jnp.int32, (BLOCK, k), 1)
    row = lax.broadcasted_iota(jnp.int32, (BLOCK, k), 0)
    for b in range(k // BLOCK):
        lo = b * BLOCK
        hi = lo + BLOCK
        r = m_ref[lo:hi, :]
        x = small_inverse(r[:, lo:hi])
        inside = jnp.logical_and(lane >= lo, lane < hi)
        r = jnp.where(inside, jnp.where(lane - lo == row, 1.0, 0.0), r)
        t = jnp.dot(beside(x), stack(r, RIGHT), preferred_element_type=F32)
        m_ref[lo:hi, :] = jnp.where(lane < hi, t, 0.0)
        if hi < k:
            left, right = stack(t, LEFT), stack(t, RIGHT)
        for at, end in ((hi, min(hi + BLOCK, k)), (hi + BLOCK, k)):
            if at < end:
                old = m_ref[at:end, :]
                column = lax.broadcasted_iota(jnp.int32, old.shape, 1)
                old = jnp.where(jnp.logical_and(column >= lo, column < hi), 0.0, old)
                m_ref[at:end, :] = old - lax.dot_general(left[:, at:end], right, TN, preferred_element_type=F32)


def finish_kernel(size, loads_ref, flags_ref, sums_ref, half_ref, parts_ref, stale_ref, p_ref, basis_ref, new_ref, out_ref, m_ref):
    live = loads_ref[0] >= 1
    refresh = jnp.logical_and(live, flags_ref[0] == 1)
    n = parts_ref.shape[0]
    k = m_ref.shape[0]
    top = k // n
    m_ref[...] = parts_ref[:, :top, :].reshape(k, k)
    upper = half_ref[...]
    lower = parts_ref[:, top:, :].sum(axis=0)
    cross = jnp.concatenate([upper[:, :128], upper[:, 128:], lower[:, :128], lower[:, 128:]], axis=0)
    lower_inverse(m_ref)
    inv = m_ref[...]
    p = p_ref[...]
    fresh = jnp.zeros(new_ref.shape, F32)
    rest = inv
    for _ in range(3):
        piece = rest.astype(BF16)
        rest = rest - piece.astype(F32)
        fresh = fresh + lax.dot_general(p, piece, NT, preferred_element_type=F32)
    old = jnp.where(live, basis_ref[...].astype(F32), 0.0)
    new_ref[...] = jnp.where(refresh, fresh, old)
    turned = jnp.dot(inv, cross, precision=HIGH, preferred_element_type=F32)
    squares = jnp.sum(sums_ref[:4, :], axis=(0, 1), keepdims=True)
    slots = jnp.sum(sums_ref[4:, :], axis=(0, 1), keepdims=True)
    scale = lax.rsqrt(squares / (slots * size) + 1e-06)
    stale = jnp.where(live, stale_ref[...], 0.0)
    out_ref[...] = jnp.where(refresh, turned, stale) * scale


def finish(size, loads, flags, sums, half, parts, stale, p, basis):
    d, k = p.shape
    return pl.pallas_call(
        functools.partial(finish_kernel, size),
        in_specs=[SM, SM] + [VM] * 6,
        out_specs=[VM, VM],
        out_shape=[jax.ShapeDtypeStruct((d, k), F32), jax.ShapeDtypeStruct((k, 128), F32)],
        scratch_shapes=[pltpu.VMEM((k, k), F32)],
        compiler_params=params(),
        cost_estimate=cost(6e9, 4 * d * k),
        name="finish",
    )(loads, flags, sums, half, parts, stale, p, basis)


def exchange(blocks, axes):
    return lax.all_to_all(blocks, axes, split_axis=0, concat_axis=0, tiled=True)


def between_planes(value):
    far = lax.axis_size(EXPERT[0])
    rows = lax.axis_size(ROW)
    pairs = [(z * rows + r, (z + r) % far * rows + r) for z in range(far) for r in range(rows)]
    return lax.ppermute(value, (EXPERT[0],) + ROW, pairs)


def both_cores(value):
    return value + lax.ppermute(value, EXPERT[1], [(0, 1), (1, 0)])


def on_device(d_whole, grads, basis, loads, flags):
    g, b = grads[0], basis[0]
    k = b.shape[1]
    s = g.shape[1]

    received = exchange(first(loads, b, g), ROW)
    n = received.shape[0]
    stale, plane, copies = spread(received, 8)
    planes = between_planes(plane)
    received, planes = lax.optimization_barrier((exchange(copies, ROW), planes))
    p, sent, rest = power(g, received, planes)
    top = k // n
    sums, half, sent = share(exchange(sent, ROW), rest, top)
    received, sums = lax.optimization_barrier((exchange(sent, ROW), both_cores(sums)))
    new_basis, rotated = finish(float(d_whole * s), loads, flags, sums, half, received, stale, p, b)
    return new_basis[None], rotated[None]


def solution(mesh):
    torus = Mesh(mesh.devices.reshape(16, 2, 4, 4), EXPERT + ROW)
    placed = (P(EXPERT, ROW, None), P(EXPERT, ROW, None), P(EXPERT), P(EXPERT))

    def whole(grads, basis, loads, flags):
        return jax.shard_map(
            functools.partial(on_device, grads.shape[1]),
            mesh=torus,
            in_specs=placed,
            out_specs=(P(EXPERT, ROW, None), P(EXPERT, None, ROW)),
            check_vma=False,
        )(grads, basis, loads, flags)

    return whole
```

```python
import functools

import jax
import jax.numpy as jnp
from jax import lax
from jax.experimental import pallas as pl
from jax.experimental.pallas import tpu as pltpu
from jax.sharding import Mesh
from jax.sharding import PartitionSpec as P

ROW = ("row_0", "row_1")
EXPERT = ("expert_0", "expert_1")
F32 = jnp.float32
BF16 = jnp.bfloat16
HIGH = lax.Precision.HIGHEST
BLOCK = 32
STAGGER = 10000
NT = (((1,), (1,)), ((), ()))
TN = (((0,), (0,)), ((), ()))
VM = pl.BlockSpec(memory_space=pltpu.VMEM)
SM = pl.BlockSpec(memory_space=pltpu.SMEM)
HBM = pl.BlockSpec(memory_space=pltpu.HBM)


def cost(flops, nbytes):
    return pl.CostEstimate(flops=int(flops), bytes_accessed=int(nbytes), transcendentals=0)


def params():
    return pltpu.CompilerParams(vmem_limit_bytes=16 * 1024 * 1024)


def product_columns(lt, g_ref, i):
    return jnp.dot(lt, g_ref[:, 256 * i : 256 * (i + 1)], preferred_element_type=F32)


def put_half(both, out_ref, i, top):
    k = both.shape[0] // 2
    for h in range(2):
        block = both[:, 128 * h : 128 * (h + 1)]
        out_ref[2 * i + h, top : top + k, :128] = block[:k, :]
        out_ref[2 * i + h, top : top + k, 128:] = block[k:, :]


def first_kernel(loads_ref, left_hbm, g_hbm, out_ref, left_ref, g_ref, sem):
    n = out_ref.shape[0]
    k = left_ref.shape[1]
    pairs = n // 2
    wide = pairs // 2
    left_copy = pltpu.make_async_copy(left_hbm, left_ref, sem.at[2])
    left_copy.start()
    loads = []
    for i in range(2):
        cols = pl.ds(256 * wide * i, 256 * wide)
        loads.append(pltpu.make_async_copy(g_hbm.at[:, cols], g_ref.at[:, cols], sem.at[i]))
        loads[-1].start()

    @pl.when(lax.axis_index(EXPERT[1]) == 0)
    def _():
        pl.delay(STAGGER)

    left_copy.wait()
    lt = left_ref[...].astype(F32).T.astype(BF16)
    squares = jnp.zeros((8, 256), F32)
    for i in range(pairs):
        if i % wide == 0:
            loads[i // wide].wait()
        both = product_columns(lt, g_ref, i)
        for h in range(2):
            out_ref[2 * i + h, :k, :] = both[:, 128 * h : 128 * (h + 1)]
        part = g_ref[:, 256 * i : 256 * (i + 1)].astype(F32)
        squares = squares + (part * part).reshape(-1, 8, 256).sum(axis=0)
    live = loads_ref[0] >= 1
    squares = squares[:, :128] + squares[:, 128:]
    squares = jnp.where(live, squares[:4, :] + squares[4:, :], 0.0)
    slot = jnp.where(live, jnp.full((4, 128), 1.0 / (4 * 128 * n), F32), 0.0)
    extra = jnp.concatenate([squares, slot], axis=0)
    for j in range(n):
        out_ref[j, k:, :] = extra


def first(loads, left, g):
    d, k = left.shape
    s = g.shape[1]
    n = s // 128
    return pl.pallas_call(
        first_kernel,
        in_specs=[SM, HBM, HBM],
        out_specs=VM,
        out_shape=jax.ShapeDtypeStruct((n, k + 8, 128), F32),
        scratch_shapes=[pltpu.VMEM((d, k), BF16), pltpu.VMEM((d, s), BF16), pltpu.SemaphoreType.DMA((3,))],
        compiler_params=params(),
        cost_estimate=cost(2 * d * k * s, 2 * d * (s + k) + 4 * k * s),
        name="first",
    )(loads, pltpu.with_memory_space_constraint(left, pltpu.HBM), pltpu.with_memory_space_constraint(g, pltpu.HBM))


def share_kernel(top, in_ref, rest_ref, sums_ref, half_ref, out_ref, wide_ref, sem):
    copies = [pltpu.make_async_copy(rest_ref, out_ref.at[:, pl.ds(top, rest_ref.shape[1]), :], sem.at[1])]
    copies[-1].start()
    total = in_ref[:, :top, :].sum(axis=0)
    wide_ref[...] = jnp.broadcast_to(total[None], wide_ref.shape)
    copies.append(pltpu.make_async_copy(wide_ref, out_ref.at[:, pl.ds(0, top), :], sem.at[0]))
    copies[-1].start()
    sums_ref[...] = in_ref[:, top : top + 8, :128].sum(axis=0)
    half_ref[...] = in_ref[:, top + 8 :, :].sum(axis=0)
    for copy in copies:
        copy.wait()


def share(parts, rest, top):
    n, r, c = parts.shape
    below = rest.shape[1]
    return pl.pallas_call(
        functools.partial(share_kernel, top),
        in_specs=[VM, VM],
        out_specs=[VM, VM, HBM],
        out_shape=[
            jax.ShapeDtypeStruct((8, 128), F32),
            jax.ShapeDtypeStruct((r - top - 8, c), F32),
            pltpu.HBM((n, top + below, c), F32),
        ],
        scratch_shapes=[pltpu.VMEM((n, top, c), F32), pltpu.SemaphoreType.DMA((2,))],
        compiler_params=params(),
        cost_estimate=cost(n * r * c, 4 * n * r * c),
        name="share",
    )(parts, rest)


def spread_kernel(in_ref, own_out, kept_ref, out_ref, own_ref, wide_ref, sem):
    rows = own_ref.shape[0]
    step = rows // 4
    copies = []
    for c in range(4):
        at = pl.ds(c * step, step)
        total = in_ref[:, at, :].sum(axis=0)
        own_ref[at, :] = total
        wide_ref[:, at, :] = jnp.broadcast_to(total[None], (wide_ref.shape[0], *total.shape))
        copies.append(pltpu.make_async_copy(wide_ref.at[:, at], out_ref.at[:, at], sem.at[c]))
        copies[-1].start()
    copies.append(pltpu.make_async_copy(own_ref, own_out, sem.at[4]))
    copies[-1].start()
    kept_ref[...] = in_ref[:, rows:, :].sum(axis=0)
    for copy in copies:
        copy.wait()


def spread(parts, kept):
    n, r, c = parts.shape
    return pl.pallas_call(
        spread_kernel,
        in_specs=[VM],
        out_specs=[HBM, VM, HBM],
        out_shape=[
            pltpu.HBM((r - kept, c), F32),
            jax.ShapeDtypeStruct((kept, c), F32),
            pltpu.HBM((n, r - kept, c), F32),
        ],
        scratch_shapes=[
            pltpu.VMEM((r - kept, c), F32),
            pltpu.VMEM((n, r - kept, c), F32),
            pltpu.SemaphoreType.DMA((5,)),
        ],
        compiler_params=params(),
        cost_estimate=cost(n * r * c, 8 * n * r * c),
        name="spread",
    )(parts)


def power_of_two(m):
    s = jnp.ones_like(m)
    for e in (64, 32, 16, 8, 4, 2, 1):
        big = m >= 2.0**e
        s = jnp.where(big, s * 2.0**-e, s)
        m = jnp.where(big, m * 2.0**-e, m)
    for e in (64, 32, 16, 8, 4, 2, 1):
        small = m < 2.0 ** (1 - e)
        s = jnp.where(small, s * 2.0 ** (e - 1), s)
        m = jnp.where(small, m * 2.0 ** (e - 1), m)
    return s


def power_kernel(g_ref, w_hbm, extra_ref, p_ref, out_ref, rest_ref, w_ref, in_sem):
    n, k, _ = w_ref.shape
    top = k // n
    step = n // 4
    loads = []
    for c in range(4):
        at = pl.ds(c * step, step)
        loads.append(pltpu.make_async_copy(w_hbm.at[at], w_ref.at[at], in_sem.at[c]))
        loads[-1].start()
    m = jnp.zeros(w_ref.shape[1:], F32)
    acc = jnp.zeros(p_ref.shape, F32)
    for j in range(0, n, 2):
        if j % step == 0:
            loads[j // step].wait()
        m = jnp.maximum(m, jnp.maximum(jnp.abs(w_ref[j]), jnp.abs(w_ref[j + 1])))
        w = jnp.concatenate([w_ref[j], w_ref[j + 1]], axis=1).astype(BF16)
        acc = acc + lax.dot_general(g_ref[:, 128 * j : 128 * j + 256], w, NT, preferred_element_type=F32)
    scale = power_of_two(jnp.max(m.T, axis=0, keepdims=True))
    acc = acc * scale
    p = acc.astype(BF16)
    p_ref[...] = p
    pt = p.astype(F32).T.astype(BF16)
    out_ref[:, :top, :] = jnp.dot(pt, p, preferred_element_type=F32).reshape(n, top, k)
    extra = jnp.concatenate([extra_ref[...], jnp.zeros((8, k - 128), F32)], axis=1)
    for j in range(n):
        out_ref[j, top : top + 8, :] = extra
    for i in range(n // 2):
        both = product_columns(pt, g_ref, i)
        put_half(both[: k // 2, :], out_ref, i, top + 8)
        put_half(both[k // 2 :, :], rest_ref, i, 0)


def power(g, w, extra):
    d, s = g.shape
    n, k, _ = w.shape
    return pl.pallas_call(
        power_kernel,
        in_specs=[VM, HBM, VM],
        out_specs=[VM, VM, VM],
        out_shape=[
            jax.ShapeDtypeStruct((d, k), BF16),
            jax.ShapeDtypeStruct((n, k // n + 8 + k // 4, k), F32),
            jax.ShapeDtypeStruct((n, k // 4, k), F32),
        ],
        scratch_shapes=[pltpu.VMEM(w.shape, F32), pltpu.SemaphoreType.DMA((4,))],
        compiler_params=params(),
        cost_estimate=cost(4 * d * k * s, 2 * d * s + 8 * k * s),
        name="power",
    )(g, pltpu.with_memory_space_constraint(w, pltpu.HBM), extra)


def sub(v, r):
    return jnp.broadcast_to(v[r : r + 1, :], v.shape)


def small_inverse(d):
    groups = BLOCK // 8
    row = lax.broadcasted_iota(jnp.int32, (8, 128), 0)
    lane = lax.broadcasted_iota(jnp.int32, (8, 128), 1)
    x = [jnp.where(lane % BLOCK == row + 8 * g, 1.0, 0.0) for g in range(groups)]
    c = [
        {g: jnp.broadcast_to(d[8 * g : 8 * g + 8, k : k + 1], (8, 128)) for g in range(k // 8, groups)}
        for k in range(BLOCK)
    ]
    for j in range(BLOCK):
        gj, sj = j // 8, j % 8
        r = lax.rsqrt(sub(c[j][gj], sj))
        inverse = r * r
        low = {g: c[j][g] * r for g in range(gj, groups)}
        for k in range(j + 1, BLOCK):
            at = sub(c[j][k // 8], k % 8) * inverse
            for g in range(k // 8, groups):
                c[k][g] = c[k][g] - c[j][g] * at
        xr = sub(x[gj], sj) * r
        below = jnp.where(row > sj, low[gj], 0.0)
        x[gj] = jnp.where(row == sj, xr, x[gj] - below * xr)
        for g in range(gj + 1, groups):
            x[g] = x[g] - low[g] * xr
    return jnp.concatenate(x, axis=0)


def pieces(x):
    high = x.astype(BF16)
    rest = x - high.astype(F32)
    mid = rest.astype(BF16)
    return high, mid, (rest - mid.astype(F32)).astype(BF16)


def stack(x, order):
    parts = pieces(x)
    return jnp.concatenate([parts[i] for i in order], axis=0)


LEFT = (0, 0, 1, 0, 2, 1)
RIGHT = (0, 1, 0, 2, 0, 1)


def beside(x):
    parts = [p.astype(F32) for p in pieces(x)]
    place = lax.broadcasted_iota(jnp.int32, x.shape, 1) // BLOCK
    per = 128 // BLOCK
    out = []
    for start in range(0, len(LEFT), per):
        wide = parts[LEFT[start]]
        for i, which in enumerate(LEFT[start : start + per]):
            wide = jnp.where(place == i, parts[which], wide)
        out.append(wide[:, : BLOCK * len(LEFT[start : start + per])])
    return jnp.concatenate(out, axis=1).astype(BF16)


def lower_inverse(m_ref):
    k = m_ref.shape[0]
    lane = lax.broadcasted_iota(jnp.int32, (BLOCK, k), 1)
    row = lax.broadcasted_iota(jnp.int32, (BLOCK, k), 0)
    for b in range(k // BLOCK):
        lo = b * BLOCK
        hi = lo + BLOCK
        r = m_ref[lo:hi, :]
        x = small_inverse(r[:, lo:hi])
        inside = jnp.logical_and(lane >= lo, lane < hi)
        r = jnp.where(inside, jnp.where(lane - lo == row, 1.0, 0.0), r)
        t = jnp.dot(beside(x), stack(r, RIGHT), preferred_element_type=F32)
        m_ref[lo:hi, :] = jnp.where(lane < hi, t, 0.0)
        if hi < k:
            left, right = stack(t, LEFT), stack(t, RIGHT)
        for at, end in ((hi, min(hi + BLOCK, k)), (hi + BLOCK, k)):
            if at < end:
                old = m_ref[at:end, :]
                column = lax.broadcasted_iota(jnp.int32, old.shape, 1)
                old = jnp.where(jnp.logical_and(column >= lo, column < hi), 0.0, old)
                m_ref[at:end, :] = old - lax.dot_general(left[:, at:end], right, TN, preferred_element_type=F32)


def finish_kernel(size, loads_ref, flags_ref, sums_ref, half_ref, parts_ref, stale_ref, p_ref, basis_ref, new_ref, out_ref, m_ref):
    live = loads_ref[0] >= 1
    refresh = jnp.logical_and(live, flags_ref[0] == 1)
    n = parts_ref.shape[0]
    k = m_ref.shape[0]
    top = k // n
    m_ref[...] = parts_ref[:, :top, :].reshape(k, k)
    upper = half_ref[...]
    lower = parts_ref[:, top:, :].sum(axis=0)
    cross = jnp.concatenate([upper[:, :128], upper[:, 128:], lower[:, :128], lower[:, 128:]], axis=0)
    lower_inverse(m_ref)
    inv = m_ref[...]
    p = p_ref[...]
    fresh = jnp.zeros(new_ref.shape, F32)
    rest = inv
    for _ in range(3):
        piece = rest.astype(BF16)
        rest = rest - piece.astype(F32)
        fresh = fresh + lax.dot_general(p, piece, NT, preferred_element_type=F32)
    old = jnp.where(live, basis_ref[...].astype(F32), 0.0)
    new_ref[...] = jnp.where(refresh, fresh, old)
    turned = jnp.dot(inv, cross, precision=HIGH, preferred_element_type=F32)
    squares = jnp.sum(sums_ref[:4, :], axis=(0, 1), keepdims=True)
    slots = jnp.sum(sums_ref[4:, :], axis=(0, 1), keepdims=True)
    scale = lax.rsqrt(squares / (slots * size) + 1e-06)
    stale = jnp.where(live, stale_ref[...], 0.0)
    out_ref[...] = jnp.where(refresh, turned, stale) * scale


def finish(size, loads, flags, sums, half, parts, stale, p, basis):
    d, k = p.shape
    return pl.pallas_call(
        functools.partial(finish_kernel, size),
        in_specs=[SM, SM] + [VM] * 6,
        out_specs=[VM, VM],
        out_shape=[jax.ShapeDtypeStruct((d, k), F32), jax.ShapeDtypeStruct((k, 128), F32)],
        scratch_shapes=[pltpu.VMEM((k, k), F32)],
        compiler_params=params(),
        cost_estimate=cost(6e9, 4 * d * k),
        name="finish",
    )(loads, flags, sums, half, parts, stale, p, basis)


def exchange(blocks, axes):
    return lax.all_to_all(blocks, axes, split_axis=0, concat_axis=0, tiled=True)


def between_planes(value):
    far = lax.axis_size(EXPERT[0])
    rows = lax.axis_size(ROW)
    pairs = [(z * rows + r, (z + r) % far * rows + r) for z in range(far) for r in range(rows)]
    return lax.ppermute(value, (EXPERT[0],) + ROW, pairs)


def both_cores(value):
    return value + lax.ppermute(value, EXPERT[1], [(0, 1), (1, 0)])


def on_device(d_whole, grads, basis, loads, flags):
    g, b = grads[0], basis[0]
    k = b.shape[1]
    s = g.shape[1]

    received = exchange(first(loads, b, g), ROW)
    n = received.shape[0]
    stale, plane, copies = spread(received, 8)
    planes = between_planes(plane)
    received, planes = lax.optimization_barrier((exchange(copies, ROW), planes))
    p, sent, rest = power(g, received, planes)
    top = k // n
    sums, half, sent = share(exchange(sent, ROW), rest, top)
    received, sums = lax.optimization_barrier((exchange(sent, ROW), both_cores(sums)))
    new_basis, rotated = finish(float(d_whole * s), loads, flags, sums, half, received, stale, p, b)
    return new_basis[None], rotated[None]


def solution(mesh):
    torus = Mesh(mesh.devices.reshape(16, 2, 4, 4), EXPERT + ROW)
    placed = (P(EXPERT, ROW, None), P(EXPERT, ROW, None), P(EXPERT), P(EXPERT))

    def whole(grads, basis, loads, flags):
        return jax.shard_map(
            functools.partial(on_device, grads.shape[1]),
            mesh=torus,
            in_specs=placed,
            out_specs=(P(EXPERT, ROW, None), P(EXPERT, None, ROW)),
            check_vma=False,
        )(grads, basis, loads, flags)

    return whole
```
